512 devices in a mesh: elem: 32 (over z, x), lev: 16 (over y, core).
Axes of the slice: x: 4, y: 8, z: 8, core: 2. Of those that a mesh axis runs over, the one named last changes fastest.
Arguments:
- cloud_state: float32 [4096, 8, 4096], P(('elem', 'lev')), may hold values from -6 to 6
- substeps: int32 [4096], P('elem'), may hold values from 4 to 16
- element_links: int32 [1024, 4], P('elem'), may hold values from 0 to 1023, as said below
- host_state: float32 [4, 64, 16384], P(None, 'lev', 'elem'), may hold values from -6 to 6
- wind_field: float32 [2, 64, 16384], P(None, 'lev', 'elem'), may hold values from -3 to 3
- node_mass: float32 [16384], P('elem'), may hold values from 0.25 to 4
- field_coupling: float32 [8, 8], replicated, may hold values from -2 to 2
- force_map: float32 [8, 4], replicated, may hold values from -3 to 3
- feedback_map: float32 [4, 8], replicated, may hold values from -5 to 5
Outputs:
- cloud_new: float32 [4096, 8, 4096], P(('elem', 'lev'))
- host_new: float32 [4, 64, 16384], P(None, 'lev', 'elem')
The draws below stay inside these ranges and needn't reach their ends.
Inputs may be any that keep to these rules, and one draw needn't show every extreme that they name: `element_links`: the 1024 elements form a doubly periodic grid of 16 rows in which each index of elem holds two neighbouring grid columns, all rows, in some order; element e lies on index e // 32 of elem. Entries 0 to 3 of row e give the global index of the element to the left, right, below and above element e. An element's right edge meets its right neighbour's left edge node for node (same j), its upper edge its upper neighbour's lower edge (same i). The left neighbour lies on the same index of elem or the one before it (cyclically), the right one on the same or the one after it, the lower and upper ones on the same index.
All inputs are finite; a program needn't handle non-finite values.
Results may differ from the reference program's by a relative error of at most 0.0003.
Values sent between devices are 32-bit elements; how exact they have to be, the bound alone decides.
No kernel may reach another device: no remote copies, remote signals or barrier semaphores. Data moves between devices by JAX's collectives and lax.ppermute only.
A program may use at most 64 MiB of HBM per device.

```python
import math
import jax
import jax.numpy as jnp
import numpy as np
from jax import lax

FIELDS = 8
CRM_X = 64
LEVELS = 64
HVARS = 4
SUB_MIN = 4
SUB_MAX = 16
COL_DEV = 128
COLS = 4096
ELEM_DEV = 32
ELEMS = 1024
ELEM_ROWS = 16
NODES = 16384
CELLS = 4096
N_ELEM = 32


def draw_substeps(key, part):
    heavy_rank = jax.random.permutation(jax.random.fold_in(key, 21), N_ELEM)
    heavy_rows = heavy_rank < max(1, N_ELEM // 8)
    strong_counts = jax.random.randint(jax.random.fold_in(key, 22), (N_ELEM, COL_DEV), SUB_MAX - 3, SUB_MAX + 1)
    weak_counts = jax.random.randint(jax.random.fold_in(key, 23), (N_ELEM, COL_DEV), SUB_MIN, SUB_MIN + 3)
    counts = jnp.where(heavy_rows[:, None], strong_counts, weak_counts)
    counts = counts.at[:, 0].set(jnp.where(heavy_rows, SUB_MAX, SUB_MIN))
    return counts.reshape(COLS).astype(jnp.int32)


def draw_element_links(key, part):
    device_keys = jax.random.split(jax.random.fold_in(key, 31), N_ELEM)
    placed = jax.vmap(lambda single: jax.random.permutation(single, ELEM_DEV))(device_keys)
    stored = jnp.argsort(placed, axis=1)
    device = jnp.arange(N_ELEM)[:, None]
    row_of = placed // 2
    side_of = placed % 2

    def global_id(dev_index, row_index, side_index):
        dev_index = (dev_index + jnp.zeros_like(row_index)) % N_ELEM
        return dev_index * ELEM_DEV + stored[dev_index, row_index % ELEM_ROWS * 2 + side_index]
    left_ids = jnp.where(side_of == 1, global_id(device, row_of, 0), global_id(device - 1, row_of, 1))
    right_ids = jnp.where(side_of == 0, global_id(device, row_of, 1), global_id(device + 1, row_of, 0))
    lower_ids = global_id(device, row_of - 1, side_of)
    upper_ids = global_id(device, row_of + 1, side_of)
    return jnp.stack([left_ids, right_ids, lower_ids, upper_ids], axis=-1).reshape(ELEMS, 4).astype(jnp.int32)


def level_of(stream_key, extent, pieces, smallest, high):
    factor_of = 1.0
    for dim, parts in pieces:
        heights = jax.random.uniform(jax.random.fold_in(jax.random.fold_in(stream_key, 6), dim), (parts,), jnp.float32, smallest / len(pieces), high / len(pieces))
        factor_of = factor_of * jnp.repeat(jnp.exp(heights), extent[dim] // parts).reshape((-1,) + (1,) * (len(extent) - 1 - dim))
    return factor_of


def normal_values(own_key, extent, width, bound, pieces=(), kind=jnp.bfloat16):
    result = width * jax.random.normal(own_key, extent, jnp.float32)
    if pieces:
        result = result * level_of(own_key, extent, pieces, -0.22, 0.18)
    return jnp.clip(result, -bound, bound).astype(kind)


def setup_inputs(seed: int = 0) -> dict:
    splits = jax.random.split(jax.random.key(seed), 10)
    return {
        "cloud_state": normal_values(splits[0], (COLS, FIELDS, CELLS), 1.0, 6.0, ((0, 512),), jnp.float32),
        "substeps": draw_substeps(jax.random.fold_in(splits[9], 71), 0),
        "element_links": draw_element_links(jax.random.fold_in(splits[9], 71), 0),
        "host_state": normal_values(splits[3], (HVARS, LEVELS, NODES), 1.0, 6.0, ((1, 16), (2, 32)), jnp.float32),
        "wind_field": normal_values(splits[4], (2, LEVELS, NODES), 0.5, 3.0, ((1, 16), (2, 32)), jnp.float32),
        "node_mass": jnp.clip(jnp.exp(math.log(4.0) - 2.7725887 * jax.random.uniform(splits[5], (NODES,), jnp.float32) ** level_of(splits[5], (NODES,), ((0, 32),), -0.2, 0.2)), 0.25, 4.0),
        "field_coupling": normal_values(splits[6], (FIELDS, FIELDS), FIELDS ** -0.5, 2.0, (), jnp.float32),
        "force_map": normal_values(splits[7], (FIELDS, HVARS), HVARS ** -0.5, 3.0, (), jnp.float32),
        "feedback_map": normal_values(splits[8], (HVARS, FIELDS), 1.0, 5.0, (), jnp.float32),
    }


lateral_mix = 0.2
vertical_mix = 0.2
cloud_step = 0.1
host_step = 0.1
host_mix = 0.2
highest = lax.Precision.HIGHEST

def gll_derivative():
    points = np.array([-1.0, -1.0 / np.sqrt(5.0), 1.0 / np.sqrt(5.0), 1.0])
    weights = np.array([1.0 / np.prod([points[index] - points[other] for other in range(4) if other != index]) for index in range(4)])
    matrix = np.zeros((4, 4))
    for target in range(4):
        for source in range(4):
            if target != source:
                matrix[target, source] = weights[source] / weights[target] / (points[target] - points[source])
        matrix[target, target] = -np.sum(matrix[target])
    return matrix

def run_clouds(cloud_state, driving, substeps, field_coupling):

    def advance(packed):
        column, forcing, count = packed
        spread = jnp.repeat(forcing, CRM_X, axis=1)
        for stepno in range(SUB_MAX):
            padded = jnp.pad(column, ((0, 0), (CRM_X, CRM_X)))
            upper_cells = padded[:, 2 * CRM_X:]
            lower_cells = padded[:, :-2 * CRM_X]
            shaped = column.reshape(FIELDS, LEVELS, CRM_X)
            eastward = jnp.roll(shaped, -1, axis=2).reshape(column.shape)
            westward = jnp.roll(shaped, 1, axis=2).reshape(column.shape)
            reaction = jnp.tanh(jnp.dot(field_coupling, column, precision=highest))
            update = column + (lateral_mix * (eastward + westward - 2.0 * column) + vertical_mix * (upper_cells + lower_cells - 2.0 * column)) + cloud_step * (reaction + spread)
            column = jnp.where(stepno < count, update, column)
        return column
    return lax.map(advance, (cloud_state, driving, substeps))

def edge_sum(quantity, element_links):
    lead, levels, count = quantity.shape
    nodes_grid = quantity.reshape(lead, levels, count // 16, 4, 4)
    from_left = jnp.take(nodes_grid[..., 3], element_links[:, 0], axis=2)
    from_right = jnp.take(nodes_grid[..., 0], element_links[:, 1], axis=2)
    nodes_grid = nodes_grid.at[..., 0].add(from_left).at[..., 3].add(from_right)
    tops = nodes_grid[..., 3, :]
    bottoms = nodes_grid[..., 0, :]
    nodes_grid = nodes_grid.at[..., 0, :].add(jnp.take(tops, element_links[:, 2], axis=2)).at[..., 3, :].add(jnp.take(bottoms, element_links[:, 3], axis=2))
    return nodes_grid.reshape(lead, levels, count)

def reference(cloud_state, substeps, element_links, host_state, wind_field, node_mass, field_coupling, force_map, feedback_map):
    pooled = host_state.reshape(HVARS, LEVELS, ELEMS, 2, 2, 2, 2).mean(axis=(4, 6))
    host_columns = pooled.reshape(HVARS, LEVELS, COLS).transpose(2, 0, 1)
    driving = jnp.einsum('fv,nvl->nfl', force_map, host_columns, precision=highest)
    cloud_new = run_clouds(cloud_state, driving, substeps, field_coupling)
    change = (cloud_new - cloud_state).reshape(COLS, FIELDS, LEVELS, CRM_X).mean(axis=3)
    column_tendency = jnp.einsum('vf,nfl->vln', feedback_map, change, precision=highest)
    physics = jnp.broadcast_to(column_tendency.reshape(HVARS, LEVELS, ELEMS, 2, 1, 2, 1), (HVARS, LEVELS, ELEMS, 2, 2, 2, 2)).reshape(HVARS, LEVELS, NODES)
    derivative = jnp.asarray(gll_derivative(), jnp.float32)

    def tendency(field):
        nodes_grid = field.reshape(HVARS, LEVELS, ELEMS, 4, 4)
        along_x = jnp.einsum('ik,vlejk->vleji', derivative, nodes_grid, precision=highest).reshape(field.shape)
        along_y = jnp.einsum('jk,vleki->vleji', derivative, nodes_grid, precision=highest).reshape(field.shape)
        padded = jnp.pad(field, ((0, 0), (1, 1), (0, 0)))
        return -(wind_field[0] * along_x + wind_field[1] * along_y) + host_mix * (padded[:, 2:] + padded[:, :-2] - 2.0 * field) + physics
    mass_total = edge_sum(node_mass.reshape(1, 1, NODES), element_links)

    def smooth(values):
        return edge_sum(node_mass * values, element_links) / mass_total
    first_section = smooth(host_state + host_step * tendency(host_state))
    second_section = smooth(0.75 * host_state + 0.25 * (first_section + host_step * tendency(first_section)))
    host_new = smooth(host_state / 3.0 + 2.0 / 3.0 * (second_section + host_step * tendency(second_section)))
    return (cloud_new, host_new)
```

```python
import jax
import jax.numpy as jnp
import numpy as np
from jax import lax
from jax.experimental import pallas as pl
from jax.experimental.pallas import tpu as pltpu
from jax.sharding import PartitionSpec as P

highest = lax.Precision.HIGHEST
F32 = jnp.float32
BF16 = jnp.bfloat16
host_step = 0.1
host_mix = 0.2
VMEM = pl.BlockSpec(memory_space=pltpu.VMEM)
SMEM = pl.BlockSpec(memory_space=pltpu.SMEM)


def gll_derivative():
    points = np.array([-1.0, -1.0 / np.sqrt(5.0), 1.0 / np.sqrt(5.0), 1.0])
    weights = np.array(
        [
            1.0 / np.prod([points[index] - points[other] for other in range(4) if other != index])
            for index in range(4)
        ]
    )
    matrix = np.zeros((4, 4))
    for target in range(4):
        for source in range(4):
            if target != source:
                matrix[target, source] = (
                    weights[source] / weights[target] / (points[target] - points[source])
                )
        matrix[target, target] = -np.sum(matrix[target])
    return matrix


def iota(shape, dim):
    return lax.broadcasted_iota(jnp.int32, shape, dim)


def dot(a, b):
    return jnp.dot(a, b, precision=highest, preferred_element_type=F32)


def ones_at(mask):
    return mask.astype(F32).astype(BF16)


def split2(values):
    top = values.astype(BF16)
    return top, (values - top.astype(F32)).astype(BF16)


def split3(values):
    top = values.astype(BF16)
    mid, low = split2(values - top.astype(F32))
    return top, mid, low


def compiler(mib=None):
    return pltpu.CompilerParams(vmem_limit_bytes=(mib or 16) * 1024 * 1024)


def pack_kernel(host_ref, wind_ref, mass_ref, links_ref, cols_ref, base_ref, up_ref, down_ref, rows):
    lev_at = lax.axis_index("lev")
    fields = jnp.concatenate([host_ref[v] for v in range(4)], axis=0)
    rows[...] = jnp.zeros_like(rows)
    rows[pl.ds(pl.multiple_of((lev_at % 8) * 16, 16), 16), :] = fields
    node = iota((128, 512), 1)
    column = node // 16 * 4 + node // 4 % 4 // 2 * 2 + node % 4 // 2
    pool = jnp.where(column == iota((128, 512), 0), 0.25, 0.0).astype(BF16)
    pooled = jnp.zeros((128, 128), F32)
    for part in split3(rows[...]):
        pooled = pooled + lax.dot_general(
            pool, part, (((1,), (1,)), ((), ())), preferred_element_type=F32
        )
    cols_ref[...] = pooled.reshape(16, 8, 128)

    mine = jnp.concatenate(
        [fields, wind_ref[0], wind_ref[1], mass_ref[...], jnp.zeros((7, 512), F32)], axis=0
    )
    source = iota((512, 512), 0)
    target = iota((512, 512), 1)
    turn = ones_at((source // 16 == target % 32) & (source % 16 == target // 32))
    moved = jnp.dot(jnp.concatenate(split3(mine), axis=0), turn, preferred_element_type=F32)
    moved = moved[:32] + (moved[32:64] + moved[64:])
    table = lax.dot_general(
        links_ref[...].astype(F32),
        (iota((32, 512), 0) == iota((32, 512), 1)).astype(F32),
        (((0,), (0,)), ((), ())),
        precision=highest,
        preferred_element_type=F32,
    )
    base_ref[...] = jnp.concatenate([moved[:25], table, jnp.zeros((3, 512), F32)], axis=0)
    up_ref[...] = jnp.concatenate(
        [moved[4 * v + 1 : 4 * v + 4] for v in range(4)]
        + [moved[16 + 4 * w + 2 : 16 + 4 * w + 4] for w in range(2)],
        axis=0,
    )
    down_ref[...] = jnp.concatenate(
        [moved[4 * v : 4 * v + 3] for v in range(4)]
        + [moved[16 + 4 * w : 16 + 4 * w + 2] for w in range(2)],
        axis=0,
    )


def pack(host_state, wind_field, node_mass, element_links):
    return pl.pallas_call(
        pack_kernel,
        out_shape=(
            jax.ShapeDtypeStruct((16, 8, 128), F32),
            jax.ShapeDtypeStruct((32, 512), F32),
            jax.ShapeDtypeStruct((16, 512), F32),
            jax.ShapeDtypeStruct((16, 512), F32),
        ),
        in_specs=[VMEM] * 4,
        out_specs=(VMEM,) * 4,
        scratch_shapes=[pltpu.VMEM((128, 512), F32)],
        compiler_params=compiler(),
        name="pack",
    )(host_state, wind_field, node_mass.reshape(1, 512), element_links)


def extend_kernel(base_ref, low_ref, high_ref, out_ref):
    base, low, high = base_ref[...], low_ref[...], high_ref[...]
    pieces = []
    for v in range(4):
        pieces += [low[3 * v + 1 : 3 * v + 3], base[4 * v : 4 * v + 4], high[3 * v : 3 * v + 2]]
    for w in range(2):
        pieces += [
            low[12 + 2 * w : 14 + 2 * w],
            base[16 + 4 * w : 20 + 4 * w],
            high[12 + 2 * w : 14 + 2 * w],
        ]
    for v in range(4):
        pieces += [low[3 * v : 3 * v + 1], high[3 * v + 2 : 3 * v + 3]]
    pieces += [base[24:32]]
    out_ref[...] = jnp.concatenate(pieces, axis=0)


def extend(base, low, high):
    return pl.pallas_call(
        extend_kernel,
        out_shape=jax.ShapeDtypeStruct((64, 512), F32),
        in_specs=[VMEM] * 3,
        out_specs=VMEM,
        compiler_params=compiler(),
        name="extend",
    )(base, low, high)


def spread_tile(tile):
    lane = iota((64, 256), 1)
    level = 2 * tile + lane // 128 + 32 * (lane % 2)
    return ones_at(iota((64, 256), 0) == level)


def cloud_kernel(
    counts_ref, cloud_ref, cols_ref, coup_ref, fmap_ref, back_ref, out_ref, tend_ref, state, parts, force
):
    lane = iota((8, 128), 1)
    low = lane < 64
    even = lane % 2 == 0
    to_pair = (lane // 2) + 64 * (lane % 2)
    from_pair = 2 * (lane % 64) + lane // 64
    first_row = lax.axis_index("lev") * 8
    counts = [counts_ref[first_row + c] for c in range(8)]
    pick_r = (iota((64, 8), 0) % 8 == iota((64, 8), 1)).astype(F32)
    pick_c = (iota((8, 64), 1) % 8 == iota((8, 64), 0)).astype(F32)
    same = iota((64, 64), 0) // 8 == iota((64, 64), 1) // 8
    coup = jnp.where(same, dot(dot(pick_r, coup_ref[...]), pick_c), 0.0) * 0.5
    c_top, c_rest = split2(coup)
    coup3 = jnp.concatenate([c_top, c_rest, c_top], axis=1)

    whole = []
    for part in range(2):
        total = cols_ref[8 * part]
        for source in range(1, 8):
            total = total + cols_ref[8 * part + source]
        whole.append(total)
    whole = jnp.concatenate(whole, axis=1)
    pick_v = (iota((4, 256), 1) % 16 // 4 == iota((4, 256), 0)).astype(F32)
    weight = dot(fmap_ref[...], pick_v)
    scaled = (
        jnp.broadcast_to(whole[:, None, :], (8, 8, 256)) * weight[None, :, :]
    ).reshape(64, 256)
    at_level = iota((256, 64), 0) // 16 * 4 + iota((256, 64), 0) % 4 == iota((256, 64), 1)
    drive = dot(scaled, at_level.astype(F32))
    drive3 = jnp.concatenate(split3(drive), axis=1)
    for tile in range(16):
        sp = spread_tile(tile)
        force[:, tile * 256 : (tile + 1) * 256] = jnp.dot(
            drive3, jnp.concatenate([sp, sp, sp], axis=0), preferred_element_type=F32
        )

    def put_parts(slot, c, q, pair):
        top, rest = split2(jnp.concatenate(pair, axis=0))
        at = slice(q * 128, (q + 1) * 128)
        parts[slot, c * 8 : c * 8 + 16, at] = top
        parts[slot, 64 + c * 8 : 80 + c * 8, at] = top
        parts[slot, 128 + c * 8 : 144 + c * 8, at] = rest

    def put_ends(slot, c, q, value):
        if q == 0:
            state[slot, c, 33] = jnp.where(even, pltpu.roll(value, 127, 1), 0.0)
        if q == 31:
            state[slot, c, 0] = jnp.where(even, 0.0, pltpu.roll(value, 1, 1))

    for c in range(0, 8, 2):
        for j in range(16):
            new = {}
            for k in (0, 1):
                a = cloud_ref[c + k, :, j * 128 : (j + 1) * 128]
                b = cloud_ref[c + k, :, (16 + j) * 128 : (17 + j) * 128]
                m0 = jnp.where(low, a, pltpu.roll(b, 64, 1))
                m1 = jnp.where(low, pltpu.roll(a, 64, 1), b)
                for h, m in ((0, m0), (1, m1)):
                    w = 2.0 * jnp.take_along_axis(m, to_pair, axis=1)
                    q = 2 * j + h
                    state[0, c + k, q + 1] = w
                    put_ends(0, c + k, q, w)
                    new[k, h] = w
            for h in (0, 1):
                put_parts(0, c, 2 * j + h, [new[0, h], new[1, h]])

    last = counts[0]
    for c in range(1, 8):
        last = jnp.maximum(last, counts[c])

    def one_step(step, carry):
        now = step % 2
        nxt = 1 - now
        for tile in range(16):
            reach = jnp.dot(
                coup3, parts[now, :, tile * 256 : (tile + 1) * 256], preferred_element_type=F32
            )
            for c in range(0, 8, 2):
                for h in (0, 1):
                    q = 2 * tile + h
                    pair = []
                    for k in (0, 1):
                        cc = c + k
                        w = state[now, cc, q + 1]
                        around = (pltpu.roll(w, 2, 1) + pltpu.roll(w, 126, 1)) + (
                            state[now, cc, q] + state[now, cc, q + 2]
                        )
                        turn = jnp.tanh(reach[cc * 8 : cc * 8 + 8, h * 128 : (h + 1) * 128])
                        push = force[cc * 8 : cc * 8 + 8, q * 128 : (q + 1) * 128]
                        new = 0.2 * ((around + w) + (turn + push))
                        new = jnp.where(step < counts[cc], new, w)
                        state[nxt, cc, q + 1] = new
                        put_ends(nxt, cc, q, new)
                        pair.append(new)
                    put_parts(nxt, c, q, pair)
        return carry

    lax.fori_loop(0, last, one_step, 0)
    end = last % 2
    for c in range(0, 8, 2):
        for j in range(16):
            diff = {}
            for k in (0, 1):
                g0 = 0.5 * jnp.take_along_axis(state[end, c + k, 2 * j + 1], from_pair, axis=1)
                g1 = 0.5 * jnp.take_along_axis(state[end, c + k, 2 * j + 2], from_pair, axis=1)
                a = jnp.where(low, g0, pltpu.roll(g1, 64, 1))
                b = jnp.where(low, pltpu.roll(g0, 64, 1), g1)
                at = slice(j * 128, (j + 1) * 128)
                bt = slice((16 + j) * 128, (17 + j) * 128)
                out_ref[c + k, :, at] = a
                out_ref[c + k, :, bt] = b
                diff[k, 0] = a - cloud_ref[c + k, :, at]
                diff[k, 1] = b - cloud_ref[c + k, :, bt]
            for h in (0, 1):
                top, rest = split2(jnp.concatenate([diff[0, h], diff[1, h]], axis=0))
                at = slice((16 * h + j) * 128, (16 * h + j + 1) * 128)
                parts[0, c * 8 : c * 8 + 16, at] = top
                parts[0, 64 + c * 8 : 80 + c * 8, at] = rest
    total = jnp.zeros((128, 64), F32)
    for tile in range(16):
        member = ones_at(iota((256, 64), 0) // 64 + 4 * tile == iota((256, 64), 1))
        total = total + jnp.dot(
            parts[0, 0:128, tile * 256 : (tile + 1) * 256], member, preferred_element_type=F32
        )
    change = (total[:64] + total[64:]) * (1.0 / 64.0)
    pick_b = (iota((32, 4), 0) // 8 == iota((32, 4), 1)).astype(F32)
    back = dot(dot(pick_b, back_ref[...]), pick_c)
    back = jnp.where(iota((32, 64), 0) % 8 == iota((32, 64), 1) // 8, back, 0.0)
    tend = dot(back, change)
    tend = jnp.concatenate(
        [
            jnp.concatenate([tend[0:8], tend[8:16]], axis=1),
            jnp.concatenate([tend[16:24], tend[24:32]], axis=1),
        ],
        axis=0,
    )
    tend_ref[...] = jnp.broadcast_to(tend[None], (32, 16, 128))


def run_clouds(counts, cloud, columns, coupling, force_map, feedback_map):
    return pl.pallas_call(
        cloud_kernel,
        out_shape=(
            jax.ShapeDtypeStruct((8, 8, 4096), F32),
            jax.ShapeDtypeStruct((32, 16, 128), F32),
        ),
        in_specs=[SMEM] + [VMEM] * 5,
        out_specs=(VMEM, VMEM),
        scratch_shapes=[
            pltpu.VMEM((2, 8, 34, 8, 128), F32),
            pltpu.VMEM((2, 192, 4096), BF16),
            pltpu.VMEM((64, 4096), F32),
        ],
        compiler_params=compiler(40),
        cost_estimate=pl.CostEstimate(
            flops=400_000_000, bytes_accessed=3_000_000, transcendentals=4_000_000
        ),
        name="clouds",
    )(counts, cloud, columns, coupling, force_map, feedback_map)


def relay_kernel(recv_ref, out_ref, near):
    at = lax.axis_index("elem")
    for d in range(5):
        near[d * 16 : (d + 1) * 16] = recv_ref[lax.rem(at + (30 + d), 32)]
    near[80:128] = jnp.zeros((48, 128), F32)
    lane = iota((16, 128), 1)
    sources = {}
    for quad in range(4):
        for half in range(2):
            pieces = []
            for d in range(5):
                for eh in range(2):
                    row = d * 16 + half * 8 + eh * 4 + quad
                    pieces.append(near[row : row + 1])
            pieces.append(jnp.zeros((6, 128), F32))
            sources[quad, half] = jnp.concatenate(pieces, axis=0)
    for target in range(16):
        level = 4 * target - 2 + lane % 8
        inside = (level >= 0) & (level < 64)
        index = lane // 8 % 2 * 64 + jnp.clip(level, 0, 63)
        total = jnp.zeros((16, 128), F32)
        for quad in range(4):
            for half in range(2):
                taken = jnp.take_along_axis(sources[quad, half], index, axis=1)
                here = (lane // 32 == quad) & (lane // 16 % 2 == half) & inside
                total = jnp.where(here, taken, total)
        out_ref[target] = total


def relay(recv):
    return pl.pallas_call(
        relay_kernel,
        out_shape=jax.ShapeDtypeStruct((16, 16, 128), F32),
        in_specs=[VMEM],
        out_specs=VMEM,
        scratch_shapes=[pltpu.VMEM((128, 128), F32)],
        compiler_params=compiler(),
        name="relay",
    )(recv)


def host_kernel(links_ref, tend_ref, e0_ref, e1_ref, e2_ref, e3_ref, e4_ref, out_ref):
    sources = (e0_ref, e1_ref, e2_ref, e3_ref, e4_ref)
    elem_at = lax.axis_index("elem")
    lev_at = lax.axis_index("lev")
    lane = iota((8, 128), 1)
    grid_row = lane // 8
    grid_col = lane % 8
    left_id = links_ref[0, 0]
    where_at = jnp.where(left_id // 32 == elem_at, left_id % 32, 0)
    lefts = []
    rights = []
    for row in range(16):
        lefts.append(where_at)
        rights.append(links_ref[where_at, 1] % 32)
        where_at = links_ref[where_at, 3] % 32
    own = jnp.zeros((8, 128), jnp.int32)
    for row in range(16):
        own = jnp.where(grid_row == row, lefts[row], own)

    def follow(ref, which, index):
        table = jnp.broadcast_to(ref[57 + which : 58 + which, 0:128], (8, 128))
        return jnp.take_along_axis(table, index, axis=1).astype(jnp.int32) % 32

    right = follow(e2_ref, 1, own)
    a2 = follow(e2_ref, 0, own)
    a1 = follow(e1_ref, 0, a2)
    a0 = follow(e1_ref, 0, a1)
    b5 = follow(e2_ref, 1, right)
    b6 = follow(e3_ref, 1, b5)
    b7 = follow(e3_ref, 1, b6)
    index = own
    for col, ids in ((0, a0), (1, a1), (2, a2), (4, right), (5, b5), (6, b6), (7, b7)):
        index = jnp.where(grid_col == col, ids, index)
    device = (grid_col + 1) // 2

    k_row = iota((256, 128), 0)
    index_w = jnp.broadcast_to(index[0:1], (256, 128))
    device_w = jnp.broadcast_to(device[0:1], (256, 128))
    chosen = ones_at((k_row % 16 // 2 == device_w) & (k_row // 16 * 2 + k_row % 2 == index_w))
    columns = jnp.zeros((128, 128), F32)
    for part in split3(tend_ref[...].reshape(256, 128).T):
        columns = columns + jnp.dot(part, chosen, preferred_element_type=F32)

    def pick(node, row):
        at = index + node % 4 * 32
        tile = slice(node // 4 * 128, node // 4 * 128 + 128)
        result = None
        for d in range(5):
            taken = jnp.take_along_axis(sources[d][row * 8 : row * 8 + 8, tile], at, axis=1)
            result = taken if result is None else jnp.where(device == d, taken, result)
        return result

    level_row = iota((8, 128), 0)
    level = 4 * lev_at - 2 + level_row
    inside = ((level >= 0) & (level < 64)).astype(F32)
    top_row = level_row == 7
    bottom_row = level_row == 0
    nodes = range(16)
    mass = [jnp.broadcast_to(pick(n, 7)[0:1], (8, 128)) for n in nodes]
    wind = [[pick(n, 4 + w) for n in nodes] for w in range(2)]
    outer = [pick(n, 6) for n in nodes]
    matrix = gll_derivative()

    def edge_sum(q):
        q = list(q)
        for j in range(4):
            first, final = q[4 * j], q[4 * j + 3]
            q[4 * j] = first + pltpu.roll(final, 1, 1)
            q[4 * j + 3] = final + pltpu.roll(first, 127, 1)
        for i in range(4):
            first, final = q[i], q[12 + i]
            q[i] = first + pltpu.roll(final, 8, 1)
            q[12 + i] = final + pltpu.roll(first, 120, 1)
        return q

    scale = [inside / total for total in edge_sum(mass)]

    def blend(terms):
        total = None
        for factor, value in terms:
            if abs(factor) < 1e-12:
                continue
            term = float(factor) * value
            total = term if total is None else total + term
        return total

    for v in range(4):
        start = [pick(n, v) for n in nodes]
        physics = [columns[quad * 32 + v * 8 : quad * 32 + v * 8 + 8] for quad in range(4)]

        def tendency(field, outermost):
            result = []
            for j in range(4):
                for i in range(4):
                    n = 4 * j + i
                    along_x = blend([(matrix[i, k], field[4 * j + k]) for k in range(4)])
                    along_y = blend([(matrix[j, k], field[4 * k + i]) for k in range(4)])
                    above = pltpu.roll(field[n], 7, 0)
                    below = pltpu.roll(field[n], 1, 0)
                    if outermost:
                        above = jnp.where(top_row, outer[n][2 * v + 1 : 2 * v + 2], above)
                        below = jnp.where(bottom_row, outer[n][2 * v : 2 * v + 1], below)
                    result.append(
                        host_mix * (above + below - 2.0 * field[n])
                        - (wind[0][n] * along_x + wind[1][n] * along_y)
                        + physics[j // 2 * 2 + i // 2]
                    )
            return result

        def smooth(values):
            total = edge_sum([mass[n] * values[n] for n in nodes])
            return [total[n] * scale[n] for n in nodes]

        rate = tendency(start, True)
        first = smooth([start[n] + host_step * rate[n] for n in nodes])
        rate = tendency(first, False)
        second = smooth(
            [0.75 * start[n] + 0.25 * (first[n] + host_step * rate[n]) for n in nodes]
        )
        rate = tendency(second, False)
        last = smooth(
            [start[n] / 3.0 + (2.0 / 3.0) * (second[n] + host_step * rate[n]) for n in nodes]
        )
        for tile in range(4):
            element = 8 * tile + lane // 16
            place = jnp.zeros((8, 128), jnp.int32)
            for row in range(16):
                place = jnp.where(element == lefts[row], 8 * row + 3, place)
                place = jnp.where(element == rights[row], 8 * row + 4, place)
            total = jnp.zeros((8, 128), F32)
            for n in nodes:
                taken = jnp.take_along_axis(last[n], place, axis=1)
                total = jnp.where(lane % 16 == n, taken, total)
            out_ref[v, :, tile * 128 : (tile + 1) * 128] = total[2:6]


def host_dynamics(links, tend, fields):
    return pl.pallas_call(
        host_kernel,
        out_shape=jax.ShapeDtypeStruct((4, 4, 512), F32),
        in_specs=[SMEM] + [VMEM] * 6,
        out_specs=VMEM,
        compiler_params=compiler(),
        name="host",
    )(links, tend, *fields)


def shards(
    cloud_state,
    substeps,
    element_links,
    host_state,
    wind_field,
    node_mass,
    field_coupling,
    force_map,
    feedback_map,
):
    def shift(value, axis, by, closed):
        count = lax.axis_size(axis)
        pairs = [(i, (i + by) % count) for i in range(count) if closed or 0 <= i + by < count]
        return lax.ppermute(value, axis, pairs)

    columns, base, up, down = pack(host_state, wind_field, node_mass, element_links)
    low = shift(up, "lev", 1, False)
    high = shift(down, "lev", -1, False)
    columns = lax.all_to_all(columns, "lev", 0, 0, tiled=True)
    own = extend(base, low, high)
    fields = [shift(own, "elem", by, True) for by in (2, 1)]
    fields += [own]
    fields += [shift(own, "elem", by, True) for by in (-1, -2)]
    cloud_new, tend = run_clouds(
        substeps, cloud_state, columns, field_coupling, force_map, feedback_map
    )
    tend = lax.all_to_all(tend, "elem", 0, 0, tiled=True)
    tend = lax.all_to_all(relay(tend), "lev", 0, 0, tiled=True)
    host_new = host_dynamics(element_links, tend, fields)
    return (cloud_new, host_new)


def solution(mesh):
    placed = (
        P(("elem", "lev"), None, None),
        P("elem"),
        P("elem", None),
        P(None, "lev", "elem"),
        P(None, "lev", "elem"),
        P("elem"),
        P(),
        P(),
        P(),
    )
    return jax.shard_map(
        shards,
        mesh=mesh,
        in_specs=placed,
        out_specs=(P(("elem", "lev"), None, None), P(None, "lev", "elem")),
        check_vma=False,
    )
```

```python
import jax
import jax.numpy as jnp
import numpy as np
from jax import lax
from jax.experimental import pallas as pl
from jax.experimental.pallas import tpu as pltpu
from jax.sharding import PartitionSpec as P

highest = lax.Precision.HIGHEST
F32 = jnp.float32
BF16 = jnp.bfloat16
host_step = 0.1
host_mix = 0.2
VMEM = pl.BlockSpec(memory_space=pltpu.VMEM)
SMEM = pl.BlockSpec(memory_space=pltpu.SMEM)


def gll_derivative():
    points = np.array([-1.0, -1.0 / np.sqrt(5.0), 1.0 / np.sqrt(5.0), 1.0])
    weights = np.array(
        [
            1.0 / np.prod([points[index] - points[other] for other in range(4) if other != index])
            for index in range(4)
        ]
    )
    matrix = np.zeros((4, 4))
    for target in range(4):
        for source in range(4):
            if target != source:
                matrix[target, source] = (
                    weights[source] / weights[target] / (points[target] - points[source])
                )
        matrix[target, target] = -np.sum(matrix[target])
    return matrix


def iota(shape, dim):
    return lax.broadcasted_iota(jnp.int32, shape, dim)


def dot(a, b):
    return jnp.dot(a, b, precision=highest, preferred_element_type=F32)


def ones_at(mask):
    return mask.astype(F32).astype(BF16)


def split2(values):
    top = values.astype(BF16)
    return top, (values - top.astype(F32)).astype(BF16)


def split3(values):
    top = values.astype(BF16)
    mid, low = split2(values - top.astype(F32))
    return top, mid, low


def compiler(mib=None):
    return pltpu.CompilerParams(vmem_limit_bytes=(mib or 16) * 1024 * 1024)


def pack_kernel(
    host_hbm, wind_hbm, mass_hbm, links_hbm, cols_ref, base_ref, up_ref, down_ref, rows, host_ref, wind_ref, mass_ref, links_ref, sems
):
    copies = [
        pltpu.make_async_copy(host_hbm, host_ref, sems.at[0]),
        pltpu.make_async_copy(wind_hbm, wind_ref, sems.at[1]),
        pltpu.make_async_copy(mass_hbm, mass_ref, sems.at[2]),
        pltpu.make_async_copy(links_hbm, links_ref, sems.at[3]),
    ]
    for copy in copies:
        copy.start()
    lev_at = lax.axis_index("lev")
    rows[...] = jnp.zeros_like(rows)
    node = iota((128, 512), 1)
    column = node // 16 * 4 + node // 4 % 4 // 2 * 2 + node % 4 // 2
    pool = jnp.where(column == iota((128, 512), 0), 0.25, 0.0).astype(BF16)
    source = iota((512, 512), 0)
    target = iota((512, 512), 1)
    turn = ones_at((source // 16 == target % 32) & (source % 16 == target // 32))
    for copy in copies:
        copy.wait()
    fields = jnp.concatenate([host_ref[v] for v in range(4)], axis=0)
    rows[pl.ds(pl.multiple_of((lev_at % 8) * 16, 16), 16), :] = fields
    pooled = jnp.zeros((128, 128), F32)
    for part in split3(rows[...]):
        pooled = pooled + lax.dot_general(
            pool, part, (((1,), (1,)), ((), ())), preferred_element_type=F32
        )
    cols_ref[...] = pooled.reshape(16, 8, 128)

    mine = jnp.concatenate(
        [fields, wind_ref[0], wind_ref[1], mass_ref[...], jnp.zeros((7, 512), F32)], axis=0
    )
    moved = jnp.dot(jnp.concatenate(split3(mine), axis=0), turn, preferred_element_type=F32)
    moved = moved[:32] + (moved[32:64] + moved[64:])
    base_ref[...] = moved
    base_ref[25:29, 0:32] = links_ref[...].astype(F32)
    up_ref[...] = jnp.concatenate(
        [moved[4 * v + 1 : 4 * v + 4] for v in range(4)]
        + [moved[16 + 4 * w + 2 : 16 + 4 * w + 4] for w in range(2)],
        axis=0,
    )
    down_ref[...] = jnp.concatenate(
        [moved[4 * v : 4 * v + 3] for v in range(4)]
        + [moved[16 + 4 * w : 16 + 4 * w + 2] for w in range(2)],
        axis=0,
    )


def pack(host_state, wind_field, node_mass, links):
    return pl.pallas_call(
        pack_kernel,
        out_shape=(
            jax.ShapeDtypeStruct((16, 8, 128), F32),
            jax.ShapeDtypeStruct((32, 512), F32),
            jax.ShapeDtypeStruct((16, 512), F32),
            jax.ShapeDtypeStruct((16, 512), F32),
        ),
        in_specs=[pl.BlockSpec(memory_space=pltpu.MemorySpace.HBM)] * 4,
        out_specs=(VMEM,) * 4,
        scratch_shapes=[
            pltpu.VMEM((128, 512), F32),
            pltpu.VMEM((4, 4, 512), F32),
            pltpu.VMEM((2, 4, 512), F32),
            pltpu.VMEM((1, 512), F32),
            pltpu.VMEM((4, 32), jnp.int32),
            pltpu.SemaphoreType.DMA((4,)),
        ],
        compiler_params=compiler(63),
        name="pack",
    )(host_state, wind_field, node_mass.reshape(1, 512), links)


def join_kernel(base_ref, low_ref, high_ref, tend_ref, out_ref):
    base, low, high = base_ref[...], low_ref[...], high_ref[...]
    pieces = []
    for v in range(4):
        pieces += [low[3 * v + 1 : 3 * v + 3], base[4 * v : 4 * v + 4], high[3 * v : 3 * v + 2]]
    for w in range(2):
        pieces += [
            low[12 + 2 * w : 14 + 2 * w],
            base[16 + 4 * w : 20 + 4 * w],
            high[12 + 2 * w : 14 + 2 * w],
        ]
    for v in range(4):
        pieces += [low[3 * v : 3 * v + 1], high[3 * v + 2 : 3 * v + 3]]
    out_ref[0:56] = jnp.concatenate(pieces, axis=0)
    out_ref[56:64] = base[24:32]
    tend = tend_ref[...].reshape(128, 128).T
    for v in range(4):
        out_ref[64:72, v * 128 : (v + 1) * 128] = tend[v * 8 : v * 8 + 8]


def join(base, low, high, tend):
    return pl.pallas_call(
        join_kernel,
        out_shape=jax.ShapeDtypeStruct((72, 512), F32),
        in_specs=[VMEM] * 4,
        out_specs=VMEM,
        compiler_params=compiler(),
        name="join",
    )(base, low, high, tend)


def swap(values, lane, bit, step):
    half = len(values) // 2
    clear = lane // step % 2 == 0
    first, second = [], []
    for a, b in zip(values[:half], values[half:]):
        first.append(jnp.where(clear, a, pltpu.roll(b, step, 1)))
        second.append(jnp.where(clear, pltpu.roll(a, 128 - step, 1), b))
    return first, second


def exchange(values, lane):
    result = []
    for part in swap(values, lane, 2, 64):
        for piece in swap(part, lane, 1, 2):
            first, second = swap(piece, lane, 0, 1)
            result += first + second
    return result


def slots(first, count=1):
    return slice(first * 128, (first + count) * 128)


def to_grid_kernel(cloud_ref, out_ref):
    lane = iota((8, 128), 1)
    index = lane % 8 // 4 * 64 + lane // 8 * 4 + lane % 4

    def one(c, carry):
        rows = pl.ds(pl.multiple_of(c * 8, 8), 8)
        for m in range(4):
            values = [cloud_ref[c, :, slots(4 * l_hi + m)] for l_hi in range(8)]
            for k, value in enumerate(exchange(values, lane)):
                out_ref[rows, slots(8 * m + k)] = 2.0 * jnp.take_along_axis(value, index, axis=1)
        return carry

    lax.fori_loop(0, 8, one, 0)


def to_grid(cloud):
    return pl.pallas_call(
        to_grid_kernel,
        out_shape=jax.ShapeDtypeStruct((64, 4096), F32),
        in_specs=[VMEM],
        out_specs=VMEM,
        compiler_params=compiler(),
        cost_estimate=pl.CostEstimate(flops=3_000_000, bytes_accessed=2_000_000, transcendentals=0),
        name="to_grid",
    )(cloud)


def from_grid_kernel(state_ref, out_ref):
    lane = iota((8, 128), 1)
    index = lane // 4 % 16 * 8 + lane // 64 * 4 + lane % 4

    def one(c, carry):
        rows = pl.ds(pl.multiple_of(c * 8, 8), 8)
        for m in range(4):
            values = [
                0.5 * jnp.take_along_axis(state_ref[rows, slots(8 * m + k + 4)], index, axis=1)
                for k in range(8)
            ]
            for l_hi, value in enumerate(exchange(values, lane)):
                out_ref[c, :, slots(4 * l_hi + m)] = value
        return carry

    lax.fori_loop(0, 8, one, 0)


def from_grid(state):
    return pl.pallas_call(
        from_grid_kernel,
        out_shape=jax.ShapeDtypeStruct((8, 8, 4096), F32),
        in_specs=[VMEM],
        out_specs=VMEM,
        compiler_params=compiler(),
        cost_estimate=pl.CostEstimate(flops=3_000_000, bytes_accessed=2_000_000, transcendentals=0),
        name="from_grid",
    )(state)


def cloud_kernel(
    counts_ref, start_ref, cols_ref, coup_ref, fmap_ref, back_ref, state_a, tend_ref, state_b, rest_a, rest_b, force
):
    lane = iota((8, 128), 1)
    first_row = lax.axis_index("lev") * 8
    counts = [counts_ref[first_row + c] for c in range(8)]
    pick_r = (iota((64, 8), 0) % 8 == iota((64, 8), 1)).astype(F32)
    pick_c = (iota((8, 64), 1) % 8 == iota((8, 64), 0)).astype(F32)
    same = iota((64, 64), 0) // 8 == iota((64, 64), 1) // 8
    coup = jnp.where(same, dot(dot(pick_r, coup_ref[...]), pick_c), 0.0) * 0.5
    c_top = coup.astype(BF16).astype(F32)
    coup3 = jnp.concatenate([c_top, coup - c_top, c_top], axis=1)

    whole = []
    for part in range(2):
        total = cols_ref[8 * part]
        for source in range(1, 8):
            total = total + cols_ref[8 * part + source]
        whole.append(total)
    whole = jnp.concatenate(whole, axis=1)
    pick_v = (iota((4, 256), 1) % 16 // 4 == iota((4, 256), 0)).astype(F32)
    weight = lax.dot_general(
        fmap_ref[...], pick_v, (((0,), (0,)), ((), ())), precision=highest, preferred_element_type=F32
    )
    scaled = (
        jnp.broadcast_to(whole[:, None, :], (8, 8, 256)) * weight[None, :, :]
    ).reshape(64, 256)
    source = iota((256, 1024), 0)
    target = iota((256, 1024), 1)
    spread = ones_at(source // 16 * 4 + source % 4 == target % 8 * 8 + target // 128)
    pushed = jnp.dot(jnp.concatenate(split3(scaled), axis=0), spread, preferred_element_type=F32)
    force[...] = pushed[:64] + (pushed[64:128] + pushed[128:])

    def put(state, rest, rows, l_lo, x_lo, value):
        at = l_lo * 4 + x_lo
        state[rows, slots(at + 4)] = value
        rest[rows, slots(at)] = value - value.astype(BF16).astype(F32)
        if l_lo == 0:
            state[rows, slots(36 + x_lo)] = jnp.where(lane % 8 == 7, 0.0, pltpu.roll(value, 127, 1))
        if l_lo == 7:
            state[rows, slots(x_lo)] = jnp.where(lane % 8 == 0, 0.0, pltpu.roll(value, 1, 1))

    def begin(c, carry):
        rows = pl.ds(pl.multiple_of(c * 8, 8), 8)
        for l_lo in range(8):
            for x_lo in range(4):
                put(state_a, rest_a, rows, l_lo, x_lo, start_ref[rows, slots(l_lo * 4 + x_lo)])
        return carry

    lax.fori_loop(0, 8, begin, 0)

    last = counts[0]
    for c in range(1, 8):
        last = jnp.maximum(last, counts[c])

    def one_step(step, old, old_rest, new, new_rest):
        for l_lo in range(8):
            reach = []
            for t in (0, 1):
                here = old[:, slots(l_lo * 4 + 2 * t + 4, 2)]
                tail = old_rest[:, slots(l_lo * 4 + 2 * t, 2)]
                reach.append(
                    jnp.dot(
                        coup3,
                        jnp.concatenate([here, here, tail], axis=0),
                        preferred_element_type=F32,
                    )
                )
            for c in range(8):
                rows = slice(c * 8, c * 8 + 8)
                centre = [old[rows, slots(l_lo * 4 + x + 4)] for x in range(4)]
                x0, x1, x2, x3 = centre
                mid = x1 + x2
                across = [
                    x0 + x1 + pltpu.roll(x3, 8, 1),
                    x0 + mid,
                    mid + x3,
                    x2 + x3 + pltpu.roll(x0, 120, 1),
                ]
                push = force[rows, slots(l_lo)]
                for x in range(4):
                    turn = jnp.tanh(reach[x // 2][rows, slots(x % 2)])
                    upright = old[rows, slots(l_lo * 4 + x)] + old[rows, slots(l_lo * 4 + x + 8)]
                    value = 0.2 * ((across[x] + upright) + (turn + push))
                    value = jnp.where(step < counts[c], value, centre[x])
                    put(new, new_rest, rows, l_lo, x, value)

    def two_steps(k, carry):
        one_step(2 * k, state_a, rest_a, state_b, rest_b)
        one_step(2 * k + 1, state_b, rest_b, state_a, rest_a)
        return carry

    lax.fori_loop(0, (last + 1) // 2, two_steps, 0)

    moved = []
    for l_lo in range(8):
        total = None
        for x in range(4):
            at = l_lo * 4 + x
            step = state_a[:, slots(at + 4)] - start_ref[:, slots(at)]
            total = step if total is None else total + step
        moved.append(total)
    moved = jnp.concatenate(moved, axis=1)
    source = iota((1024, 128), 0)
    member = ones_at(source % 8 * 8 + source // 128 == iota((1024, 128), 1))
    summed = jnp.dot(jnp.concatenate(split3(moved), axis=0), member, preferred_element_type=F32)
    change = (summed[:64] + (summed[64:128] + summed[128:])) * (1.0 / 128.0)

    source = iota((128, 512), 0)
    target = iota((128, 512), 1)
    window = ones_at(source == target // 32 * 4 - 2 + target % 8)
    wide = jnp.dot(jnp.concatenate(split3(change), axis=0), window, preferred_element_type=F32)
    wide = wide[:64] + (wide[64:128] + wide[128:])
    pick_v = (iota((4, 512), 1) % 32 // 8 == iota((4, 512), 0)).astype(F32)
    weight = lax.dot_general(
        back_ref[...], pick_v, (((0,), (0,)), ((), ())), precision=highest, preferred_element_type=F32
    )
    tend = (wide.reshape(8, 8, 512) * weight[None]).sum(axis=1)
    for target in range(16):
        piece = tend[:, slots(target // 4)]
        if target % 4:
            piece = pltpu.roll(piece, 128 - target % 4 * 32, 1)
        tend_ref[target] = piece


def run_clouds(counts, start, columns, coupling, force_map, feedback_map):
    return pl.pallas_call(
        cloud_kernel,
        out_shape=(
            jax.ShapeDtypeStruct((64, 40 * 128), F32),
            jax.ShapeDtypeStruct((16, 8, 128), F32),
        ),
        in_specs=[SMEM] + [VMEM] * 5,
        out_specs=(VMEM, VMEM),
        scratch_shapes=[
            pltpu.VMEM((64, 40 * 128), F32),
            pltpu.VMEM((64, 4096), F32),
            pltpu.VMEM((64, 4096), F32),
            pltpu.VMEM((64, 1024), F32),
        ],
        compiler_params=compiler(24),
        cost_estimate=pl.CostEstimate(
            flops=400_000_000, bytes_accessed=3_000_000, transcendentals=4_000_000
        ),
        name="clouds",
    )(counts, start, columns, coupling, force_map, feedback_map)


def host_kernel(links_ref, e0_ref, e1_ref, e2_ref, e3_ref, e4_ref, out_ref, start, field, rate, aux):
    sources = (e0_ref, e1_ref, e2_ref, e3_ref, e4_ref)
    elem_at = lax.axis_index("elem")
    lev_at = lax.axis_index("lev")
    lane = iota((8, 128), 1)
    grid_row = lane // 8
    grid_col = lane % 8
    left_id = links_ref[0, 0]
    where_at = jnp.where(left_id // 32 == elem_at, left_id % 32, 0)
    lefts = []
    rights = []
    for row in range(16):
        lefts.append(where_at)
        rights.append(links_ref[1, where_at] % 32)
        where_at = links_ref[3, where_at] % 32
    own = jnp.zeros((8, 128), jnp.int32)
    for row in range(16):
        own = jnp.where(grid_row == row, lefts[row], own)

    def follow(ref, which, index):
        table = jnp.broadcast_to(ref[57 + which : 58 + which, 0:128], (8, 128))
        return jnp.take_along_axis(table, index, axis=1).astype(jnp.int32) % 32

    right = follow(e2_ref, 1, own)
    a2 = follow(e2_ref, 0, own)
    a1 = follow(e1_ref, 0, a2)
    a0 = follow(e1_ref, 0, a1)
    b5 = follow(e2_ref, 1, right)
    b6 = follow(e3_ref, 1, b5)
    b7 = follow(e3_ref, 1, b6)
    index = own
    for col, ids in ((0, a0), (1, a1), (2, a2), (4, right), (5, b5), (6, b6), (7, b7)):
        index = jnp.where(grid_col == col, ids, index)
    device = (grid_col + 1) // 2

    def pick(node, row):
        at = index + node % 4 * 32
        tile = slice(node // 4 * 128, node // 4 * 128 + 128)
        result = None
        for d in range(5):
            taken = jnp.take_along_axis(sources[d][row * 8 : row * 8 + 8, tile], at, axis=1)
            result = taken if result is None else jnp.where(device == d, taken, result)
        return result

    def column_rate(v, quad):
        result = None
        for d in range(5):
            taken = jnp.take_along_axis(sources[d][64:72, slots(v)], index * 4 + quad, axis=1)
            result = taken if result is None else jnp.where(device == d, taken, result)
        return result

    level_row = iota((8, 128), 0)
    level = 4 * lev_at - 2 + level_row
    inside = ((level >= 0) & (level < 64)).astype(F32)
    top_row = level_row == 7
    bottom_row = level_row == 0
    nodes = range(16)
    matrix = gll_derivative()

    def edge_sum(q):
        q = list(q)
        for j in range(4):
            first, final = q[4 * j], q[4 * j + 3]
            q[4 * j] = first + pltpu.roll(final, 1, 1)
            q[4 * j + 3] = final + pltpu.roll(first, 127, 1)
        for i in range(4):
            first, final = q[i], q[12 + i]
            q[i] = first + pltpu.roll(final, 8, 1)
            q[12 + i] = final + pltpu.roll(first, 120, 1)
        return q

    mass = [jnp.broadcast_to(pick(n, 7)[0:1], (8, 128)) for n in nodes]
    scale = [inside / total for total in edge_sum(mass)]
    for n in nodes:
        aux[0, n] = mass[n]
        aux[1, n] = scale[n]
        aux[2, n] = pick(n, 4)
        aux[3, n] = pick(n, 5)
        aux[4, n] = pick(n, 6)
        for v in range(4):
            value = pick(n, v)
            start[v, n] = value
            field[v, n] = value
    for v in range(4):
        for quad in range(4):
            rate[v, quad] = column_rate(v, quad)

    def blend(terms):
        total = None
        for factor, value in terms:
            if abs(factor) < 1e-12:
                continue
            term = float(factor) * value
            total = term if total is None else total + term
        return total

    def stage(number, carry):
        keep = jnp.where(number == 0, 0.0, jnp.where(number == 1, 0.75, 1.0 / 3.0))
        take = jnp.where(number == 0, 1.0, jnp.where(number == 1, 0.25, 2.0 / 3.0))
        for v in range(4):
            now = [field[v, n] for n in nodes]
            weighted = []
            for j in range(4):
                for i in range(4):
                    n = 4 * j + i
                    along_x = blend([(matrix[i, k], now[4 * j + k]) for k in range(4)])
                    along_y = blend([(matrix[j, k], now[4 * k + i]) for k in range(4)])
                    above = jnp.where(top_row, aux[4, n, 2 * v + 1 : 2 * v + 2], pltpu.roll(now[n], 7, 0))
                    below = jnp.where(bottom_row, aux[4, n, 2 * v : 2 * v + 1], pltpu.roll(now[n], 1, 0))
                    tendency = (
                        host_mix * (above + below - 2.0 * now[n])
                        - (aux[2, n] * along_x + aux[3, n] * along_y)
                        + rate[v, j // 2 * 2 + i // 2]
                    )
                    value = keep * start[v, n] + take * (now[n] + host_step * tendency)
                    weighted.append(aux[0, n] * value)
            for n, total in enumerate(edge_sum(weighted)):
                field[v, n] = total * aux[1, n]
        return carry

    lax.fori_loop(0, 3, stage, 0)
    for tile in range(4):
        element = 8 * tile + lane // 16
        place = jnp.zeros((8, 128), jnp.int32)
        for row in range(16):
            place = jnp.where(element == lefts[row], 8 * row + 3, place)
            place = jnp.where(element == rights[row], 8 * row + 4, place)
        for v in range(4):
            total = jnp.zeros((8, 128), F32)
            for n in nodes:
                taken = jnp.take_along_axis(field[v, n], place, axis=1)
                total = jnp.where(lane % 16 == n, taken, total)
            out_ref[v, :, tile * 128 : (tile + 1) * 128] = total[2:6]


def host_dynamics(links, fields):
    return pl.pallas_call(
        host_kernel,
        out_shape=jax.ShapeDtypeStruct((4, 4, 512), F32),
        in_specs=[SMEM] + [VMEM] * 5,
        out_specs=VMEM,
        scratch_shapes=[
            pltpu.VMEM((4, 16, 8, 128), F32),
            pltpu.VMEM((4, 16, 8, 128), F32),
            pltpu.VMEM((4, 4, 8, 128), F32),
            pltpu.VMEM((5, 16, 8, 128), F32),
        ],
        compiler_params=compiler(),
        name="host",
    )(links, *fields)


def shards(
    cloud_state,
    substeps,
    element_links,
    host_state,
    wind_field,
    node_mass,
    field_coupling,
    force_map,
    feedback_map,
):
    def shift(value, axis, by, closed):
        count = lax.axis_size(axis)
        pairs = [(i, (i + by) % count) for i in range(count) if closed or 0 <= i + by < count]
        return lax.ppermute(value, axis, pairs)

    links = element_links.T
    columns, base, up, down = pack(host_state, wind_field, node_mass, links)
    low = shift(up, "lev", 1, False)
    high = shift(down, "lev", -1, False)
    columns = lax.all_to_all(columns, "lev", 0, 0, tiled=True)
    state, tend = run_clouds(
        substeps, to_grid(cloud_state), columns, field_coupling, force_map.T, feedback_map
    )
    tend = lax.all_to_all(tend, "lev", 0, 0, tiled=True)
    own = join(base, low, high, tend)
    fields = [shift(own, "elem", by, True) for by in (2, 1)]
    fields += [own]
    fields += [shift(own, "elem", by, True) for by in (-1, -2)]
    cloud_new = from_grid(state)
    host_new = host_dynamics(links, fields)
    return (cloud_new, host_new)


def solution(mesh):
    placed = (
        P(("elem", "lev"), None, None),
        P("elem"),
        P("elem", None),
        P(None, "lev", "elem"),
        P(None, "lev", "elem"),
        P("elem"),
        P(),
        P(),
        P(),
    )
    return jax.shard_map(
        shards,
        mesh=mesh,
        in_specs=placed,
        out_specs=(P(("elem", "lev"), None, None), P(None, "lev", "elem")),
        check_vma=False,
    )
```

```python
import jax
import jax.numpy as jnp
import numpy as np
from jax import lax
from jax.experimental import pallas as pl
from jax.experimental.pallas import tpu as pltpu
from jax.sharding import PartitionSpec as P

highest = lax.Precision.HIGHEST
F32 = jnp.float32
BF16 = jnp.bfloat16
host_step = 0.1
host_mix = 0.2
VMEM = pl.BlockSpec(memory_space=pltpu.VMEM)
SMEM = pl.BlockSpec(memory_space=pltpu.SMEM)


def gll_derivative():
    points = np.array([-1.0, -1.0 / np.sqrt(5.0), 1.0 / np.sqrt(5.0), 1.0])
    weights = np.array(
        [
            1.0 / np.prod([points[index] - points[other] for other in range(4) if other != index])
            for index in range(4)
        ]
    )
    matrix = np.zeros((4, 4))
    for target in range(4):
        for source in range(4):
            if target != source:
                matrix[target, source] = (
                    weights[source] / weights[target] / (points[target] - points[source])
                )
        matrix[target, target] = -np.sum(matrix[target])
    return matrix


def iota(shape, dim):
    return lax.broadcasted_iota(jnp.int32, shape, dim)


def dot(a, b):
    return jnp.dot(a, b, precision=highest, preferred_element_type=F32)


def ones_at(mask):
    return mask.astype(F32).astype(BF16)


def split2(values):
    top = values.astype(BF16)
    return top, (values - top.astype(F32)).astype(BF16)


def split3(values):
    top = values.astype(BF16)
    mid, low = split2(values - top.astype(F32))
    return top, mid, low


def compiler(mib=None):
    return pltpu.CompilerParams(vmem_limit_bytes=(mib or 16) * 1024 * 1024)


def pack_kernel(
    host_hbm, wind_hbm, mass_hbm, links_hbm, cols_ref, base_ref, up_ref, down_ref, rows, host_ref, wind_ref, mass_ref, links_ref, sems
):
    copies = [
        pltpu.make_async_copy(host_hbm, host_ref, sems.at[0]),
        pltpu.make_async_copy(wind_hbm, wind_ref, sems.at[1]),
        pltpu.make_async_copy(mass_hbm, mass_ref, sems.at[2]),
        pltpu.make_async_copy(links_hbm, links_ref, sems.at[3]),
    ]
    for copy in copies:
        copy.start()
    lev_at = lax.axis_index("lev")
    rows[...] = jnp.zeros_like(rows)
    node = iota((128, 512), 1)
    column = node // 16 * 4 + node // 4 % 4 // 2 * 2 + node % 4 // 2
    pool = jnp.where(column == iota((128, 512), 0), 0.25, 0.0).astype(BF16)
    source = iota((512, 512), 0)
    target = iota((512, 512), 1)
    turn = ones_at((source // 16 == target % 32) & (source % 16 == target // 32))
    for copy in copies:
        copy.wait()
    fields = jnp.concatenate([host_ref[v] for v in range(4)], axis=0)
    rows[pl.ds(pl.multiple_of((lev_at % 8) * 16, 16), 16), :] = fields
    pooled = jnp.zeros((128, 128), F32)
    for part in split3(rows[...]):
        pooled = pooled + lax.dot_general(
            pool, part, (((1,), (1,)), ((), ())), preferred_element_type=F32
        )
    cols_ref[...] = pooled.reshape(16, 8, 128)

    mine = jnp.concatenate(
        [fields, wind_ref[0], wind_ref[1], mass_ref[...], jnp.zeros((7, 512), F32)], axis=0
    )
    moved = jnp.dot(jnp.concatenate(split3(mine), axis=0), turn, preferred_element_type=F32)
    moved = moved[:32] + (moved[32:64] + moved[64:])
    base_ref[...] = moved
    base_ref[25:29, 0:32] = links_ref[...].astype(F32)
    up_ref[...] = jnp.concatenate(
        [moved[4 * v + 1 : 4 * v + 4] for v in range(4)]
        + [moved[16 + 4 * w + 2 : 16 + 4 * w + 4] for w in range(2)],
        axis=0,
    )
    down_ref[...] = jnp.concatenate(
        [moved[4 * v : 4 * v + 3] for v in range(4)]
        + [moved[16 + 4 * w : 16 + 4 * w + 2] for w in range(2)],
        axis=0,
    )


def pack(host_state, wind_field, node_mass, links):
    return pl.pallas_call(
        pack_kernel,
        out_shape=(
            jax.ShapeDtypeStruct((16, 8, 128), F32),
            jax.ShapeDtypeStruct((32, 512), F32),
            jax.ShapeDtypeStruct((16, 512), F32),
            jax.ShapeDtypeStruct((16, 512), F32),
        ),
        in_specs=[pl.BlockSpec(memory_space=pltpu.MemorySpace.HBM)] * 4,
        out_specs=(VMEM,) * 4,
        scratch_shapes=[
            pltpu.VMEM((128, 512), F32),
            pltpu.VMEM((4, 4, 512), F32),
            pltpu.VMEM((2, 4, 512), F32),
            pltpu.VMEM((1, 512), F32),
            pltpu.VMEM((4, 32), jnp.int32),
            pltpu.SemaphoreType.DMA((4,)),
        ],
        compiler_params=compiler(63),
        name="pack",
    )(host_state, wind_field, node_mass.reshape(1, 512), links)


def join_kernel(base_ref, low_ref, high_ref, tend_ref, out_ref):
    base, low, high = base_ref[...], low_ref[...], high_ref[...]
    pieces = []
    for v in range(4):
        pieces += [low[3 * v + 1 : 3 * v + 3], base[4 * v : 4 * v + 4], high[3 * v : 3 * v + 2]]
    for w in range(2):
        pieces += [
            low[12 + 2 * w : 14 + 2 * w],
            base[16 + 4 * w : 20 + 4 * w],
            high[12 + 2 * w : 14 + 2 * w],
        ]
    for v in range(4):
        pieces += [low[3 * v : 3 * v + 1], high[3 * v + 2 : 3 * v + 3]]
    out_ref[0:56] = jnp.concatenate(pieces, axis=0)
    out_ref[56:64] = base[24:32]
    tend = tend_ref[...].reshape(128, 128).T
    for v in range(4):
        out_ref[64:72, v * 128 : (v + 1) * 128] = tend[v * 8 : v * 8 + 8]


def join(base, low, high, tend):
    return pl.pallas_call(
        join_kernel,
        out_shape=jax.ShapeDtypeStruct((72, 512), F32),
        in_specs=[VMEM] * 4,
        out_specs=VMEM,
        compiler_params=compiler(),
        name="join",
    )(base, low, high, tend)


def swap(values, lane, bit, step):
    half = len(values) // 2
    clear = lane // step % 2 == 0
    first, second = [], []
    for a, b in zip(values[:half], values[half:]):
        first.append(jnp.where(clear, a, pltpu.roll(b, step, 1)))
        second.append(jnp.where(clear, pltpu.roll(a, 128 - step, 1), b))
    return first, second


def exchange(values, lane):
    result = []
    for part in swap(values, lane, 2, 64):
        for piece in swap(part, lane, 1, 2):
            first, second = swap(piece, lane, 0, 1)
            result += first + second
    return result


def slots(first, count=1):
    return slice(first * 128, (first + count) * 128)


def put(state, rows, l_lo, x_lo, value, lane):
    at = l_lo * 4 + x_lo
    state[rows, slots(at + 4)] = value
    if l_lo == 0:
        state[rows, slots(36 + x_lo)] = jnp.where(lane % 8 == 7, 0.0, pltpu.roll(value, 127, 1))
    if l_lo == 7:
        state[rows, slots(x_lo)] = jnp.where(lane % 8 == 0, 0.0, pltpu.roll(value, 1, 1))


def to_grid_kernel(cloud_ref, out_ref):
    lane = iota((8, 128), 1)
    index = lane % 8 // 4 * 64 + lane // 8 * 4 + lane % 4

    def one(c, carry):
        rows = pl.ds(pl.multiple_of(c * 8, 8), 8)
        for m in range(4):
            values = [cloud_ref[c, :, slots(4 * l_hi + m)] for l_hi in range(8)]
            for k, value in enumerate(exchange(values, lane)):
                value = 2.0 * jnp.take_along_axis(value, index, axis=1)
                put(out_ref, rows, 2 * m + k // 4, k % 4, value, lane)
        return carry

    lax.fori_loop(0, 8, one, 0)


def to_grid(cloud):
    return pl.pallas_call(
        to_grid_kernel,
        out_shape=jax.ShapeDtypeStruct((64, 40 * 128), F32),
        in_specs=[VMEM],
        out_specs=VMEM,
        compiler_params=compiler(),
        cost_estimate=pl.CostEstimate(flops=3_000_000, bytes_accessed=2_000_000, transcendentals=0),
        name="to_grid",
    )(cloud)


def from_grid_kernel(state_ref, out_ref):
    lane = iota((8, 128), 1)
    index = lane // 4 % 16 * 8 + lane // 64 * 4 + lane % 4

    def one(c, carry):
        rows = pl.ds(pl.multiple_of(c * 8, 8), 8)
        for m in range(4):
            values = [
                0.5 * jnp.take_along_axis(state_ref[rows, slots(8 * m + k + 4)], index, axis=1)
                for k in range(8)
            ]
            for l_hi, value in enumerate(exchange(values, lane)):
                out_ref[c, :, slots(4 * l_hi + m)] = value
        return carry

    lax.fori_loop(0, 8, one, 0)


def from_grid(state):
    return pl.pallas_call(
        from_grid_kernel,
        out_shape=jax.ShapeDtypeStruct((8, 8, 4096), F32),
        in_specs=[VMEM],
        out_specs=VMEM,
        compiler_params=compiler(),
        cost_estimate=pl.CostEstimate(flops=3_000_000, bytes_accessed=2_000_000, transcendentals=0),
        name="from_grid",
    )(state)


def cloud_kernel(
    counts_ref, start_ref, cols_ref, coup_ref, fmap_ref, back_ref, state_a, tend_ref, state_b, force
):
    lane = iota((8, 128), 1)
    first_row = lax.axis_index("lev") * 8
    counts = [counts_ref[first_row + c] for c in range(8)]
    pick_r = (iota((64, 8), 0) % 8 == iota((64, 8), 1)).astype(F32)
    pick_c = (iota((8, 64), 1) % 8 == iota((8, 64), 0)).astype(F32)
    same = iota((64, 64), 0) // 8 == iota((64, 64), 1) // 8
    coup = jnp.where(same, dot(dot(pick_r, coup_ref[...]), pick_c), 0.0) * 0.5
    c_top, c_rest = split2(coup)
    coup3 = jnp.concatenate([c_top, c_rest, c_top], axis=1)

    pick_v = (iota((4, 256), 1) % 16 // 4 == iota((4, 256), 0)).astype(F32)
    drive = lax.dot_general(
        fmap_ref[...], pick_v, (((0,), (0,)), ((), ())), precision=highest, preferred_element_type=F32
    )
    whole = []
    for part in range(2):
        total = cols_ref[8 * part]
        for source in range(1, 8):
            total = total + cols_ref[8 * part + source]
        whole.append(total)
    whole = jnp.concatenate(whole, axis=1)
    scaled = (
        jnp.broadcast_to(whole[:, None, :], (8, 8, 256)) * drive[None]
    ).reshape(64, 256)
    source = iota((256, 1024), 0)
    target = iota((256, 1024), 1)
    spread = ones_at(source // 16 * 4 + source % 4 == target % 8 * 8 + target // 128)
    pushed = jnp.dot(jnp.concatenate(split3(scaled), axis=0), spread, preferred_element_type=F32)
    force[...] = pushed[:64] + (pushed[64:128] + pushed[128:])

    def begin(c, carry):
        rows = pl.ds(pl.multiple_of(c * 8, 8), 8)
        state_a[rows, :] = start_ref[rows, :]
        return carry

    lax.fori_loop(0, 8, begin, 0)

    last = counts[0]
    for c in range(1, 8):
        last = jnp.maximum(last, counts[c])

    def one_step(step, old, new):
        for l_lo in range(8):
            for t in (0, 1):
                top, rest = split2(old[:, slots(l_lo * 4 + 2 * t + 4, 2)])
                reach = jnp.dot(
                    coup3,
                    jnp.concatenate([top, top, rest], axis=0),
                    preferred_element_type=F32,
                )
                for c in range(8):
                    rows = slice(c * 8, c * 8 + 8)
                    x0, x1, x2, x3 = [old[rows, slots(l_lo * 4 + x + 4)] for x in range(4)]
                    push = force[rows, slots(l_lo)]
                    if t == 0:
                        pair = x0 + x1
                        across = [pair + pltpu.roll(x3, 8, 1), pair + x2]
                        centre = [x0, x1]
                    else:
                        pair = x2 + x3
                        across = [pair + x1, pair + pltpu.roll(x0, 120, 1)]
                        centre = [x2, x3]
                    for k in (0, 1):
                        x = 2 * t + k
                        turn = jnp.tanh(reach[rows, slots(k)])
                        upright = old[rows, slots(l_lo * 4 + x)] + old[rows, slots(l_lo * 4 + x + 8)]
                        value = 0.2 * ((across[k] + upright) + (turn + push))
                        value = jnp.where(step < counts[c], value, centre[k])
                        put(new, rows, l_lo, x, value, lane)

    def two_steps(k, carry):
        one_step(2 * k, state_a, state_b)
        one_step(2 * k + 1, state_b, state_a)
        return carry

    lax.fori_loop(0, (last + 1) // 2, two_steps, 0)

    moved = []
    for l_lo in range(8):
        total = None
        for x in range(4):
            at = l_lo * 4 + x + 4
            step = state_a[:, slots(at)] - start_ref[:, slots(at)]
            total = step if total is None else total + step
        moved.append(total)
    moved = jnp.concatenate(moved, axis=1)
    source = iota((1024, 128), 0)
    member = ones_at(source % 8 * 8 + source // 128 == iota((1024, 128), 1))
    summed = jnp.dot(jnp.concatenate(split3(moved), axis=0), member, preferred_element_type=F32)
    change = (summed[:64] + (summed[64:128] + summed[128:])) * (1.0 / 128.0)
    source = iota((128, 512), 0)
    target = iota((128, 512), 1)
    window = ones_at(source == target // 32 * 4 - 2 + target % 8)
    wide = jnp.dot(jnp.concatenate(split3(change), axis=0), window, preferred_element_type=F32)
    wide = wide[:64] + (wide[64:128] + wide[128:])
    pick_v = (iota((4, 512), 1) % 32 // 8 == iota((4, 512), 0)).astype(F32)
    weight = lax.dot_general(
        back_ref[...], pick_v, (((0,), (0,)), ((), ())), precision=highest, preferred_element_type=F32
    )
    tend = (wide.reshape(8, 8, 512) * weight[None]).sum(axis=1)
    for target in range(16):
        piece = tend[:, slots(target // 4)]
        if target % 4:
            piece = pltpu.roll(piece, 128 - target % 4 * 32, 1)
        tend_ref[target] = piece


def run_clouds(counts, start, columns, coupling, force_map, feedback_map):
    return pl.pallas_call(
        cloud_kernel,
        out_shape=(
            jax.ShapeDtypeStruct((64, 40 * 128), F32),
            jax.ShapeDtypeStruct((16, 8, 128), F32),
        ),
        in_specs=[SMEM] + [VMEM] * 5,
        out_specs=(VMEM, VMEM),
        scratch_shapes=[
            pltpu.VMEM((64, 40 * 128), F32),
            pltpu.VMEM((64, 1024), F32),
        ],
        compiler_params=pltpu.CompilerParams(
            vmem_limit_bytes=24 * 1024 * 1024
        ),
        cost_estimate=pl.CostEstimate(
            flops=400_000_000, bytes_accessed=3_000_000, transcendentals=4_000_000
        ),
        name="clouds",
    )(counts, start, columns, coupling, force_map, feedback_map)


def host_kernel(links_ref, own_ref, e1_ref, e2_ref, e3_ref, e4_ref, out_ref, start, field, rate, aux):
    elem_at = lax.axis_index("elem")
    lev_at = lax.axis_index("lev")
    even = elem_at % 2 == 0
    lower = elem_at // 2 % 2 == 0
    sources = (
        (own_ref, 2),
        (e1_ref, jnp.where(even, 3, 1)),
        (e2_ref, jnp.where(even, 1, 3)),
        (e3_ref, jnp.where(lower, 4, 0)),
        (e4_ref, jnp.where(lower, 0, 4)),
    )
    lane = iota((8, 128), 1)
    grid_row = lane // 8
    grid_col = lane % 8
    left_id = links_ref[0, 0]
    where_at = jnp.where(left_id // 32 == elem_at, left_id % 32, 0)
    lefts = []
    rights = []
    for row in range(16):
        lefts.append(where_at)
        rights.append(links_ref[1, where_at] % 32)
        where_at = links_ref[3, where_at] % 32
    own = jnp.zeros((8, 128), jnp.int32)
    for row in range(16):
        own = jnp.where(grid_row == row, lefts[row], own)

    def table(ref, which):
        return jnp.broadcast_to(ref[57 + which : 58 + which, 0:128], (8, 128))

    def follow(values, index):
        return jnp.take_along_axis(values, index, axis=1).astype(jnp.int32) % 32

    own_left, own_right = table(own_ref, 0), table(own_ref, 1)
    far_left = jnp.where(even, table(e2_ref, 0), table(e1_ref, 0))
    far_right = jnp.where(even, table(e1_ref, 1), table(e2_ref, 1))
    right = follow(own_right, own)
    a2 = follow(own_left, own)
    a1 = follow(far_left, a2)
    a0 = follow(far_left, a1)
    b5 = follow(own_right, right)
    b6 = follow(far_right, b5)
    b7 = follow(far_right, b6)
    index = own
    for col, ids in ((0, a0), (1, a1), (2, a2), (4, right), (5, b5), (6, b6), (7, b7)):
        index = jnp.where(grid_col == col, ids, index)
    device = (grid_col + 1) // 2

    def pick(node, row):
        at = index + node % 4 * 32
        tile = slice(node // 4 * 128, node // 4 * 128 + 128)
        result = None
        for ref, d in sources:
            taken = jnp.take_along_axis(ref[row * 8 : row * 8 + 8, tile], at, axis=1)
            result = taken if result is None else jnp.where(device == d, taken, result)
        return result

    def column_rate(v, quad):
        result = None
        for ref, d in sources:
            taken = jnp.take_along_axis(ref[64:72, slots(v)], index * 4 + quad, axis=1)
            result = taken if result is None else jnp.where(device == d, taken, result)
        return result

    level_row = iota((8, 128), 0)
    level = 4 * lev_at - 2 + level_row
    inside = ((level >= 0) & (level < 64)).astype(F32)
    top_row = level_row == 7
    bottom_row = level_row == 0
    nodes = range(16)
    matrix = gll_derivative()

    def edge_sum(q):
        q = list(q)
        for j in range(4):
            first, final = q[4 * j], q[4 * j + 3]
            q[4 * j] = first + pltpu.roll(final, 1, 1)
            q[4 * j + 3] = final + pltpu.roll(first, 127, 1)
        for i in range(4):
            first, final = q[i], q[12 + i]
            q[i] = first + pltpu.roll(final, 8, 1)
            q[12 + i] = final + pltpu.roll(first, 120, 1)
        return q

    mass = [jnp.broadcast_to(pick(n, 7)[0:1], (8, 128)) for n in nodes]
    scale = [inside / total for total in edge_sum(mass)]
    for n in nodes:
        aux[0, n] = mass[n]
        aux[1, n] = scale[n]
        aux[2, n] = pick(n, 4)
        aux[3, n] = pick(n, 5)
        aux[4, n] = pick(n, 6)
        for v in range(4):
            value = pick(n, v)
            start[v, n] = value
            field[v, n] = value
    for v in range(4):
        for quad in range(4):
            rate[v, quad] = column_rate(v, quad)

    def blend(terms):
        total = None
        for factor, value in terms:
            if abs(factor) < 1e-12:
                continue
            term = float(factor) * value
            total = term if total is None else total + term
        return total

    def stage(number, carry):
        keep = jnp.where(number == 0, 0.0, jnp.where(number == 1, 0.75, 1.0 / 3.0))
        take = jnp.where(number == 0, 1.0, jnp.where(number == 1, 0.25, 2.0 / 3.0))
        for v in range(4):
            now = [field[v, n] for n in nodes]
            weighted = []
            for j in range(4):
                for i in range(4):
                    n = 4 * j + i
                    along_x = blend([(matrix[i, k], now[4 * j + k]) for k in range(4)])
                    along_y = blend([(matrix[j, k], now[4 * k + i]) for k in range(4)])
                    above = jnp.where(top_row, aux[4, n, 2 * v + 1 : 2 * v + 2], pltpu.roll(now[n], 7, 0))
                    below = jnp.where(bottom_row, aux[4, n, 2 * v : 2 * v + 1], pltpu.roll(now[n], 1, 0))
                    tendency = (
                        host_mix * (above + below - 2.0 * now[n])
                        - (aux[2, n] * along_x + aux[3, n] * along_y)
                        + rate[v, j // 2 * 2 + i // 2]
                    )
                    value = keep * start[v, n] + take * (now[n] + host_step * tendency)
                    weighted.append(aux[0, n] * value)
            for n, total in enumerate(edge_sum(weighted)):
                field[v, n] = total * aux[1, n]
        return carry

    lax.fori_loop(0, 3, stage, 0)
    for tile in range(4):
        element = 8 * tile + lane // 16
        place = jnp.zeros((8, 128), jnp.int32)
        for row in range(16):
            place = jnp.where(element == lefts[row], 8 * row + 3, place)
            place = jnp.where(element == rights[row], 8 * row + 4, place)
        for v in range(4):
            total = jnp.zeros((8, 128), F32)
            for n in nodes:
                taken = jnp.take_along_axis(field[v, n], place, axis=1)
                total = jnp.where(lane % 16 == n, taken, total)
            out_ref[v, :, tile * 128 : (tile + 1) * 128] = total[2:6]


def host_dynamics(links, fields):
    return pl.pallas_call(
        host_kernel,
        out_shape=jax.ShapeDtypeStruct((4, 4, 512), F32),
        in_specs=[SMEM] + [VMEM] * 5,
        out_specs=VMEM,
        scratch_shapes=[
            pltpu.VMEM((4, 16, 8, 128), F32),
            pltpu.VMEM((4, 16, 8, 128), F32),
            pltpu.VMEM((4, 4, 8, 128), F32),
            pltpu.VMEM((5, 16, 8, 128), F32),
        ],
        compiler_params=compiler(),
        name="host",
    )(links, *fields)


def shards(
    cloud_state,
    substeps,
    element_links,
    host_state,
    wind_field,
    node_mass,
    field_coupling,
    force_map,
    feedback_map,
):
    def shift(value, axis, by, closed):
        count = lax.axis_size(axis)
        pairs = [(i, (i + by) % count) for i in range(count) if closed or 0 <= i + by < count]
        return lax.ppermute(value, axis, pairs)

    links = element_links.T
    columns, base, up, down = pack(host_state, wind_field, node_mass, links)
    low = shift(up, "lev", 1, False)
    high = shift(down, "lev", -1, False)
    columns = lax.all_to_all(columns, "lev", 0, 0, tiled=True)
    state, tend = run_clouds(
        substeps, to_grid(cloud_state), columns, field_coupling, force_map.T, feedback_map
    )
    tend = lax.all_to_all(tend, "lev", 0, 0, tiled=True)
    own = join(base, low, high, tend)
    fields = [own]
    for step in (1, 2):
        for odd in (0, 1):
            pairs = []
            for i in range(32):
                up = (i // step + odd) % 2 == 0
                pairs.append((i, (i + step) % 32 if up else (i - step) % 32))
            fields.append(lax.ppermute(own, "elem", pairs))
    cloud_new = from_grid(state)
    host_new = host_dynamics(links, fields)
    return (cloud_new, host_new)


def solution(mesh):
    placed = (
        P(("elem", "lev"), None, None),
        P("elem"),
        P("elem", None),
        P(None, "lev", "elem"),
        P(None, "lev", "elem"),
        P("elem"),
        P(),
        P(),
        P(),
    )
    return jax.shard_map(
        shards,
        mesh=mesh,
        in_specs=placed,
        out_specs=(P(("elem", "lev"), None, None), P(None, "lev", "elem")),
        check_vma=False,
    )
```

```python
import jax
import jax.numpy as jnp
import numpy as np
from jax import lax
from jax.experimental import pallas as pl
from jax.experimental.pallas import tpu as pltpu
from jax.sharding import PartitionSpec as P

highest = lax.Precision.HIGHEST
COLUMNS = 2
F32 = jnp.float32
BF16 = jnp.bfloat16
host_step = 0.1
host_mix = 0.2
VMEM = pl.BlockSpec(memory_space=pltpu.VMEM)
SMEM = pl.BlockSpec(memory_space=pltpu.SMEM)


def gll_derivative():
    points = np.array([-1.0, -1.0 / np.sqrt(5.0), 1.0 / np.sqrt(5.0), 1.0])
    weights = np.array(
        [
            1.0 / np.prod([points[index] - points[other] for other in range(4) if other != index])
            for index in range(4)
        ]
    )
    matrix = np.zeros((4, 4))
    for target in range(4):
        for source in range(4):
            if target != source:
                matrix[target, source] = (
                    weights[source] / weights[target] / (points[target] - points[source])
                )
        matrix[target, target] = -np.sum(matrix[target])
    return matrix


def iota(shape, dim):
    return lax.broadcasted_iota(jnp.int32, shape, dim)


def dot(a, b):
    return jnp.dot(a, b, precision=highest, preferred_element_type=F32)


def ones_at(mask):
    return mask.astype(F32).astype(BF16)


def split2(values):
    top = values.astype(BF16)
    return top, (values - top.astype(F32)).astype(BF16)


def split3(values):
    top = values.astype(BF16)
    mid, low = split2(values - top.astype(F32))
    return top, mid, low


def compiler(mib=None):
    return pltpu.CompilerParams(vmem_limit_bytes=(mib or 16) * 1024 * 1024)


def pack_kernel(
    host_hbm, wind_hbm, mass_hbm, links_hbm, cols_ref, base_ref, up_ref, down_ref, rows, host_ref, wind_ref, mass_ref, links_ref, sems
):
    copies = [
        pltpu.make_async_copy(host_hbm, host_ref, sems.at[0]),
        pltpu.make_async_copy(wind_hbm, wind_ref, sems.at[1]),
        pltpu.make_async_copy(mass_hbm, mass_ref, sems.at[2]),
        pltpu.make_async_copy(links_hbm, links_ref, sems.at[3]),
    ]
    for copy in copies:
        copy.start()
    lev_at = lax.axis_index("lev")
    rows[...] = jnp.zeros_like(rows)
    node = iota((128, 512), 1)
    column = node // 16 * 4 + node // 4 % 4 // 2 * 2 + node % 4 // 2
    pool = jnp.where(column == iota((128, 512), 0), 0.25, 0.0).astype(BF16)
    source = iota((512, 512), 0)
    target = iota((512, 512), 1)
    turn = ones_at((source // 16 == target % 32) & (source % 16 == target // 32))
    for copy in copies:
        copy.wait()
    fields = jnp.concatenate([host_ref[v] for v in range(4)], axis=0)
    rows[pl.ds(pl.multiple_of((lev_at % 8) * 16, 16), 16), :] = fields
    pooled = jnp.zeros((128, 128), F32)
    for part in split3(rows[...]):
        pooled = pooled + lax.dot_general(
            pool, part, (((1,), (1,)), ((), ())), preferred_element_type=F32
        )
    cols_ref[...] = pooled.reshape(16, 8, 128)

    mine = jnp.concatenate(
        [fields, wind_ref[0], wind_ref[1], mass_ref[...], jnp.zeros((7, 512), F32)], axis=0
    )
    moved = jnp.dot(jnp.concatenate(split3(mine), axis=0), turn, preferred_element_type=F32)
    moved = moved[:32] + (moved[32:64] + moved[64:])
    base_ref[...] = moved
    base_ref[25:29, 0:32] = links_ref[...].astype(F32)
    up_ref[...] = jnp.concatenate(
        [moved[4 * v + 1 : 4 * v + 4] for v in range(4)]
        + [moved[16 + 4 * w + 2 : 16 + 4 * w + 4] for w in range(2)],
        axis=0,
    )
    down_ref[...] = jnp.concatenate(
        [moved[4 * v : 4 * v + 3] for v in range(4)]
        + [moved[16 + 4 * w : 16 + 4 * w + 2] for w in range(2)],
        axis=0,
    )


def pack(host_state, wind_field, node_mass, links):
    return pl.pallas_call(
        pack_kernel,
        out_shape=(
            jax.ShapeDtypeStruct((16, 8, 128), F32),
            jax.ShapeDtypeStruct((32, 512), F32),
            jax.ShapeDtypeStruct((16, 512), F32),
            jax.ShapeDtypeStruct((16, 512), F32),
        ),
        in_specs=[pl.BlockSpec(memory_space=pltpu.MemorySpace.HBM)] * 4,
        out_specs=(VMEM,) * 4,
        scratch_shapes=[
            pltpu.VMEM((128, 512), F32),
            pltpu.VMEM((4, 4, 512), F32),
            pltpu.VMEM((2, 4, 512), F32),
            pltpu.VMEM((1, 512), F32),
            pltpu.VMEM((4, 32), jnp.int32),
            pltpu.SemaphoreType.DMA((4,)),
        ],
        compiler_params=compiler(63),
        name="pack",
    )(host_state, wind_field, node_mass.reshape(1, 512), links)


def join_kernel(base_ref, low_ref, high_ref, tend_ref, out_ref):
    base, low, high = base_ref[...], low_ref[...], high_ref[...]
    pieces = []
    for v in range(4):
        pieces += [low[3 * v + 1 : 3 * v + 3], base[4 * v : 4 * v + 4], high[3 * v : 3 * v + 2]]
    for w in range(2):
        pieces += [
            low[12 + 2 * w : 14 + 2 * w],
            base[16 + 4 * w : 20 + 4 * w],
            high[12 + 2 * w : 14 + 2 * w],
        ]
    for v in range(4):
        pieces += [low[3 * v : 3 * v + 1], high[3 * v + 2 : 3 * v + 3]]
    out_ref[0:56] = jnp.concatenate(pieces, axis=0)
    out_ref[56:64] = base[24:32]
    tend = tend_ref[...].reshape(128, 128).T
    for v in range(4):
        out_ref[64:72, v * 128 : (v + 1) * 128] = tend[v * 8 : v * 8 + 8]


def join(base, low, high, tend):
    return pl.pallas_call(
        join_kernel,
        out_shape=jax.ShapeDtypeStruct((72, 512), F32),
        in_specs=[VMEM] * 4,
        out_specs=VMEM,
        compiler_params=compiler(),
        name="join",
    )(base, low, high, tend)


def swap(values, lane, bit, step):
    half = len(values) // 2
    clear = lane // step % 2 == 0
    first, second = [], []
    for a, b in zip(values[:half], values[half:]):
        first.append(jnp.where(clear, a, pltpu.roll(b, step, 1)))
        second.append(jnp.where(clear, pltpu.roll(a, 128 - step, 1), b))
    return first, second


def exchange(values, lane):
    result = []
    for part in swap(values, lane, 2, 64):
        for piece in swap(part, lane, 1, 2):
            first, second = swap(piece, lane, 0, 1)
            result += first + second
    return result


def slots(first, count=1):
    return slice(first * 128, (first + count) * 128)


def put(state, rows, l_lo, x_lo, value, lane):
    at = l_lo * 4 + x_lo
    state[rows, slots(at + 4)] = value
    if l_lo == 0:
        state[rows, slots(36 + x_lo)] = jnp.where(lane % 8 == 7, 0.0, pltpu.roll(value, 127, 1))
    if l_lo == 7:
        state[rows, slots(x_lo)] = jnp.where(lane % 8 == 0, 0.0, pltpu.roll(value, 1, 1))


def to_grid_kernel(cloud_ref, out_ref):
    lane = iota((8, 128), 1)
    index = lane % 8 // 4 * 64 + lane // 8 * 4 + lane % 4

    def some(trip, carry):
        for m in range(4):
            for part in range(COLUMNS):
                c = trip * COLUMNS + part
                rows = pl.ds(pl.multiple_of(c * 8, 8), 8)
                values = [cloud_ref[c, :, slots(4 * l_hi + m)] for l_hi in range(8)]
                for k, value in enumerate(exchange(values, lane)):
                    value = 2.0 * jnp.take_along_axis(value, index, axis=1)
                    put(out_ref, rows, 2 * m + k // 4, k % 4, value, lane)
        return carry

    lax.fori_loop(0, 8 // COLUMNS, some, 0)


def to_grid(cloud):
    return pl.pallas_call(
        to_grid_kernel,
        out_shape=jax.ShapeDtypeStruct((64, 40 * 128), F32),
        in_specs=[VMEM],
        out_specs=VMEM,
        compiler_params=compiler(),
        cost_estimate=pl.CostEstimate(flops=3_000_000, bytes_accessed=2_000_000, transcendentals=0),
        name="to_grid",
    )(cloud)


def from_grid_kernel(state_ref, out_hbm, columns, sems):
    lane = iota((8, 128), 1)
    index = lane // 4 % 16 * 8 + lane // 64 * 4 + lane % 4

    def copy(c):
        return pltpu.make_async_copy(columns.at[c], out_hbm.at[c], sems.at[c])

    def some(trip, carry):
        for m in range(4):
            for part in range(COLUMNS):
                c = trip * COLUMNS + part
                rows = pl.ds(pl.multiple_of(c * 8, 8), 8)
                values = [
                    0.5 * jnp.take_along_axis(state_ref[rows, slots(8 * m + k + 4)], index, axis=1)
                    for k in range(8)
                ]
                for l_hi, value in enumerate(exchange(values, lane)):
                    columns[c, :, slots(4 * l_hi + m)] = value
        for part in range(COLUMNS):
            copy(trip * COLUMNS + part).start()
        return carry

    lax.fori_loop(0, 8 // COLUMNS, some, 0)
    for c in range(8):
        copy(c).wait()


def from_grid(state):
    return pl.pallas_call(
        from_grid_kernel,
        out_shape=jax.ShapeDtypeStruct((8, 8, 4096), F32),
        in_specs=[VMEM],
        out_specs=pl.BlockSpec(memory_space=pl.ANY),
        scratch_shapes=[pltpu.VMEM((8, 8, 4096), F32), pltpu.SemaphoreType.DMA((8,))],
        compiler_params=compiler(),
        cost_estimate=pl.CostEstimate(flops=3_000_000, bytes_accessed=2_000_000, transcendentals=0),
        name="from_grid",
    )(state)


def cloud_kernel(
    counts_ref, start_ref, cols_ref, coup_ref, fmap_ref, back_ref, state_a, tend_ref, state_b, force
):
    lane = iota((8, 128), 1)
    first_row = lax.axis_index("lev") * 8
    counts = [counts_ref[first_row + c] for c in range(8)]
    pick_r = (iota((64, 8), 0) % 8 == iota((64, 8), 1)).astype(F32)
    pick_c = (iota((8, 64), 1) % 8 == iota((8, 64), 0)).astype(F32)
    same = iota((64, 64), 0) // 8 == iota((64, 64), 1) // 8
    coup = jnp.where(same, dot(dot(pick_r, coup_ref[...]), pick_c), 0.0) * 0.5
    c_top, c_rest = split2(coup)
    coup3 = jnp.concatenate([c_top, c_rest, c_top], axis=1)

    pick_v = (iota((4, 256), 1) % 16 // 4 == iota((4, 256), 0)).astype(F32)
    drive = lax.dot_general(
        fmap_ref[...], pick_v, (((0,), (0,)), ((), ())), precision=highest, preferred_element_type=F32
    )
    whole = []
    for part in range(2):
        total = cols_ref[8 * part]
        for source in range(1, 8):
            total = total + cols_ref[8 * part + source]
        whole.append(total)
    whole = jnp.concatenate(whole, axis=1)
    scaled = (
        jnp.broadcast_to(whole[:, None, :], (8, 8, 256)) * drive[None]
    ).reshape(64, 256)
    source = iota((256, 1024), 0)
    target = iota((256, 1024), 1)
    spread = ones_at(source // 16 * 4 + source % 4 == target % 8 * 8 + target // 128)
    pushed = jnp.dot(jnp.concatenate(split3(scaled), axis=0), spread, preferred_element_type=F32)
    force[...] = pushed[:64] + (pushed[64:128] + pushed[128:])

    def begin(c, carry):
        rows = pl.ds(pl.multiple_of(c * 8, 8), 8)
        state_a[rows, :] = start_ref[rows, :]
        return carry

    lax.fori_loop(0, 8, begin, 0)

    last = counts[0]
    for c in range(1, 8):
        last = jnp.maximum(last, counts[c])

    def one_step(step, old, new):
        for l_lo in range(8):
            for t in (0, 1):
                top, rest = split2(old[:, slots(l_lo * 4 + 2 * t + 4, 2)])
                reach = jnp.dot(
                    coup3,
                    jnp.concatenate([top, top, rest], axis=0),
                    preferred_element_type=F32,
                )
                for c in range(8):
                    rows = slice(c * 8, c * 8 + 8)
                    x0, x1, x2, x3 = [old[rows, slots(l_lo * 4 + x + 4)] for x in range(4)]
                    push = force[rows, slots(l_lo)]
                    if t == 0:
                        pair = x0 + x1
                        across = [pair + pltpu.roll(x3, 8, 1), pair + x2]
                        centre = [x0, x1]
                    else:
                        pair = x2 + x3
                        across = [pair + x1, pair + pltpu.roll(x0, 120, 1)]
                        centre = [x2, x3]
                    for k in (0, 1):
                        x = 2 * t + k
                        turn = jnp.tanh(reach[rows, slots(k)])
                        upright = old[rows, slots(l_lo * 4 + x)] + old[rows, slots(l_lo * 4 + x + 8)]
                        value = 0.2 * ((across[k] + upright) + (turn + push))
                        value = jnp.where(step < counts[c], value, centre[k])
                        put(new, rows, l_lo, x, value, lane)

    def two_steps(k, carry):
        one_step(2 * k, state_a, state_b)
        one_step(2 * k + 1, state_b, state_a)
        return carry

    lax.fori_loop(0, (last + 1) // 2, two_steps, 0)

    moved = []
    for l_lo in range(8):
        total = None
        for x in range(4):
            at = l_lo * 4 + x + 4
            step = state_a[:, slots(at)] - start_ref[:, slots(at)]
            total = step if total is None else total + step
        moved.append(total)
    moved = jnp.concatenate(moved, axis=1)
    source = iota((1024, 128), 0)
    member = ones_at(source % 8 * 8 + source // 128 == iota((1024, 128), 1))
    summed = jnp.dot(jnp.concatenate(split3(moved), axis=0), member, preferred_element_type=F32)
    change = (summed[:64] + (summed[64:128] + summed[128:])) * (1.0 / 128.0)
    source = iota((128, 512), 0)
    target = iota((128, 512), 1)
    window = ones_at(source == target // 32 * 4 - 2 + target % 8)
    wide = jnp.dot(jnp.concatenate(split3(change), axis=0), window, preferred_element_type=F32)
    wide = wide[:64] + (wide[64:128] + wide[128:])
    pick_v = (iota((4, 512), 1) % 32 // 8 == iota((4, 512), 0)).astype(F32)
    weight = lax.dot_general(
        back_ref[...], pick_v, (((0,), (0,)), ((), ())), precision=highest, preferred_element_type=F32
    )
    tend = (wide.reshape(8, 8, 512) * weight[None]).sum(axis=1)
    for target in range(16):
        piece = tend[:, slots(target // 4)]
        if target % 4:
            piece = pltpu.roll(piece, 128 - target % 4 * 32, 1)
        tend_ref[target] = piece


def run_clouds(counts, start, columns, coupling, force_map, feedback_map):
    return pl.pallas_call(
        cloud_kernel,
        out_shape=(
            jax.ShapeDtypeStruct((64, 40 * 128), F32),
            jax.ShapeDtypeStruct((16, 8, 128), F32),
        ),
        in_specs=[SMEM] + [VMEM] * 5,
        out_specs=(VMEM, VMEM),
        scratch_shapes=[
            pltpu.VMEM((64, 40 * 128), F32),
            pltpu.VMEM((64, 1024), F32),
        ],
        compiler_params=pltpu.CompilerParams(
            vmem_limit_bytes=24 * 1024 * 1024
        ),
        cost_estimate=pl.CostEstimate(
            flops=400_000_000, bytes_accessed=3_000_000, transcendentals=4_000_000
        ),
        name="clouds",
    )(counts, start, columns, coupling, force_map, feedback_map)


def host_kernel(links_ref, own_ref, e1_ref, e2_ref, e3_ref, e4_ref, out_ref, start, field, rate, aux):
    elem_at = lax.axis_index("elem")
    lev_at = lax.axis_index("lev")
    even = elem_at % 2 == 0
    lower = elem_at // 2 % 2 == 0
    sources = (
        (own_ref, 2),
        (e1_ref, jnp.where(even, 3, 1)),
        (e2_ref, jnp.where(even, 1, 3)),
        (e3_ref, jnp.where(lower, 4, 0)),
        (e4_ref, jnp.where(lower, 0, 4)),
    )
    lane = iota((8, 128), 1)
    grid_row = lane // 8
    grid_col = lane % 8
    left_id = links_ref[0, 0]
    where_at = jnp.where(left_id // 32 == elem_at, left_id % 32, 0)
    lefts = []
    rights = []
    for row in range(16):
        lefts.append(where_at)
        rights.append(links_ref[1, where_at] % 32)
        where_at = links_ref[3, where_at] % 32
    own = jnp.zeros((8, 128), jnp.int32)
    for row in range(16):
        own = jnp.where(grid_row == row, lefts[row], own)

    def table(ref, which):
        return jnp.broadcast_to(ref[57 + which : 58 + which, 0:128], (8, 128))

    def follow(values, index):
        return jnp.take_along_axis(values, index, axis=1).astype(jnp.int32) % 32

    own_left, own_right = table(own_ref, 0), table(own_ref, 1)
    far_left = jnp.where(even, table(e2_ref, 0), table(e1_ref, 0))
    far_right = jnp.where(even, table(e1_ref, 1), table(e2_ref, 1))
    right = follow(own_right, own)
    a2 = follow(own_left, own)
    a1 = follow(far_left, a2)
    a0 = follow(far_left, a1)
    b5 = follow(own_right, right)
    b6 = follow(far_right, b5)
    b7 = follow(far_right, b6)
    index = own
    for col, ids in ((0, a0), (1, a1), (2, a2), (4, right), (5, b5), (6, b6), (7, b7)):
        index = jnp.where(grid_col == col, ids, index)
    device = (grid_col + 1) // 2

    def pick(node, row):
        at = index + node % 4 * 32
        tile = slice(node // 4 * 128, node // 4 * 128 + 128)
        result = None
        for ref, d in sources:
            taken = jnp.take_along_axis(ref[row * 8 : row * 8 + 8, tile], at, axis=1)
            result = taken if result is None else jnp.where(device == d, taken, result)
        return result

    def column_rate(v, quad):
        result = None
        for ref, d in sources:
            taken = jnp.take_along_axis(ref[64:72, slots(v)], index * 4 + quad, axis=1)
            result = taken if result is None else jnp.where(device == d, taken, result)
        return result

    level_row = iota((8, 128), 0)
    level = 4 * lev_at - 2 + level_row
    inside = ((level >= 0) & (level < 64)).astype(F32)
    top_row = level_row == 7
    bottom_row = level_row == 0
    nodes = range(16)
    matrix = gll_derivative()

    def edge_sum(q):
        q = list(q)
        for j in range(4):
            first, final = q[4 * j], q[4 * j + 3]
            q[4 * j] = first + pltpu.roll(final, 1, 1)
            q[4 * j + 3] = final + pltpu.roll(first, 127, 1)
        for i in range(4):
            first, final = q[i], q[12 + i]
            q[i] = first + pltpu.roll(final, 8, 1)
            q[12 + i] = final + pltpu.roll(first, 120, 1)
        return q

    mass = [jnp.broadcast_to(pick(n, 7)[0:1], (8, 128)) for n in nodes]
    scale = [inside / total for total in edge_sum(mass)]
    for n in nodes:
        aux[0, n] = mass[n]
        aux[1, n] = scale[n]
        aux[2, n] = pick(n, 4)
        aux[3, n] = pick(n, 5)
        aux[4, n] = pick(n, 6)
        for v in range(4):
            value = pick(n, v)
            start[v, n] = value
            field[v, n] = value
    for v in range(4):
        for quad in range(4):
            rate[v, quad] = column_rate(v, quad)

    def blend(terms):
        total = None
        for factor, value in terms:
            if abs(factor) < 1e-12:
                continue
            term = float(factor) * value
            total = term if total is None else total + term
        return total

    def stage(number, carry):
        keep = jnp.where(number == 0, 0.0, jnp.where(number == 1, 0.75, 1.0 / 3.0))
        take = jnp.where(number == 0, 1.0, jnp.where(number == 1, 0.25, 2.0 / 3.0))
        for v in range(4):
            now = [field[v, n] for n in nodes]
            weighted = []
            for j in range(4):
                for i in range(4):
                    n = 4 * j + i
                    along_x = blend([(matrix[i, k], now[4 * j + k]) for k in range(4)])
                    along_y = blend([(matrix[j, k], now[4 * k + i]) for k in range(4)])
                    above = jnp.where(top_row, aux[4, n, 2 * v + 1 : 2 * v + 2], pltpu.roll(now[n], 7, 0))
                    below = jnp.where(bottom_row, aux[4, n, 2 * v : 2 * v + 1], pltpu.roll(now[n], 1, 0))
                    tendency = (
                        host_mix * (above + below - 2.0 * now[n])
                        - (aux[2, n] * along_x + aux[3, n] * along_y)
                        + rate[v, j // 2 * 2 + i // 2]
                    )
                    value = keep * start[v, n] + take * (now[n] + host_step * tendency)
                    weighted.append(aux[0, n] * value)
            for n, total in enumerate(edge_sum(weighted)):
                field[v, n] = total * aux[1, n]
        return carry

    lax.fori_loop(0, 3, stage, 0)
    for tile in range(4):
        element = 8 * tile + lane // 16
        place = jnp.zeros((8, 128), jnp.int32)
        for row in range(16):
            place = jnp.where(element == lefts[row], 8 * row + 3, place)
            place = jnp.where(element == rights[row], 8 * row + 4, place)
        for v in range(4):
            total = jnp.zeros((8, 128), F32)
            for n in nodes:
                taken = jnp.take_along_axis(field[v, n], place, axis=1)
                total = jnp.where(lane % 16 == n, taken, total)
            out_ref[v, :, tile * 128 : (tile + 1) * 128] = total[2:6]


def host_dynamics(links, fields):
    return pl.pallas_call(
        host_kernel,
        out_shape=jax.ShapeDtypeStruct((4, 4, 512), F32),
        in_specs=[SMEM] + [VMEM] * 5,
        out_specs=VMEM,
        scratch_shapes=[
            pltpu.VMEM((4, 16, 8, 128), F32),
            pltpu.VMEM((4, 16, 8, 128), F32),
            pltpu.VMEM((4, 4, 8, 128), F32),
            pltpu.VMEM((5, 16, 8, 128), F32),
        ],
        compiler_params=compiler(),
        name="host",
    )(links, *fields)


def shards(
    cloud_state,
    substeps,
    element_links,
    host_state,
    wind_field,
    node_mass,
    field_coupling,
    force_map,
    feedback_map,
):
    def shift(value, axis, by, closed):
        count = lax.axis_size(axis)
        pairs = [(i, (i + by) % count) for i in range(count) if closed or 0 <= i + by < count]
        return lax.ppermute(value, axis, pairs)

    links = element_links.T
    columns, base, up, down = pack(host_state, wind_field, node_mass, links)
    low = shift(up, "lev", 1, False)
    high = shift(down, "lev", -1, False)
    columns = lax.all_to_all(columns, "lev", 0, 0, tiled=True)
    state, tend = run_clouds(
        substeps, to_grid(cloud_state), columns, field_coupling, force_map.T, feedback_map
    )
    tend = lax.all_to_all(tend, "lev", 0, 0, tiled=True)
    own = join(base, low, high, tend)
    fields = [own]
    for step in (1, 2):
        for odd in (0, 1):
            pairs = []
            for i in range(32):
                up = (i // step + odd) % 2 == 0
                pairs.append((i, (i + step) % 32 if up else (i - step) % 32))
            fields.append(lax.ppermute(own, "elem", pairs))
    cloud_new = from_grid(state)
    host_new = host_dynamics(links, fields)
    return (cloud_new, host_new)


def solution(mesh):
    placed = (
        P(("elem", "lev"), None, None),
        P("elem"),
        P("elem", None),
        P(None, "lev", "elem"),
        P(None, "lev", "elem"),
        P("elem"),
        P(),
        P(),
        P(),
    )
    return jax.shard_map(
        shards,
        mesh=mesh,
        in_specs=placed,
        out_specs=(P(("elem", "lev"), None, None), P(None, "lev", "elem")),
        check_vma=False,
    )
```
